128 devices in a mesh: tp: 4 (over x), dp: 32 (over z, y, core).
Axes of the slice: x: 4, y: 4, z: 4, core: 2. Of those that a mesh axis runs over, the one named last changes fastest.
Arguments:
- hidden: bfloat16 [128, 128, 4096], P('dp')
- positions: int32 [128], replicated
- ln1_gain: bfloat16 [4096], replicated
- ln1_bias: bfloat16 [4096], replicated
- w_q: bfloat16 [4096, 6144], P(None, 'tp')
- w_k: bfloat16 [4096, 1024], P(None, 'tp')
- w_v: bfloat16 [4096, 1024], P(None, 'tp')
- w_o: bfloat16 [6144, 4096], P('tp')
- ln2_gain: bfloat16 [4096], replicated
- ln2_bias: bfloat16 [4096], replicated
- w_up: bfloat16 [4096, 16384], P(None, 'tp')
- w_down: bfloat16 [16384, 4096], P('tp')
Outputs:
- output 1: bfloat16 [128, 128, 4096], P('dp')
- output 2: float32 [16384], P('tp')
- output 3: float32 [48], P('tp')
- output 4: float32 [4096], replicated
All inputs are finite; a program needn't handle non-finite values.
Results may differ from the reference program's by a relative error of at most 0.0101698.
Values sent between devices are 32-bit elements.
A program may use at most 1 GiB of HBM per device.

```python
import jax
import jax.numpy as jnp
from jax import lax

D = 4096
HEADS = 48
KV_HEADS = 8
HEAD = 128
FF = 16384
SAMPLES = 128
SEQ_LEN = 128
POS_GAP = 64
ROT_DIM = HEAD // 2
ROPE_BASE = 10000.0
LN_EPS = 1e-5


def setup_inputs(seed: int = 0) -> dict:
    key_list = jax.random.split(jax.random.key(seed), 13)
    sample_shift = jax.random.normal(key_list[0], (SAMPLES, 1, D), jnp.float32)
    token_noise = jax.random.normal(key_list[1], (SAMPLES, SEQ_LEN, D), jnp.float32)
    hidden = (0.8 * sample_shift + 0.6 * token_noise).astype(jnp.bfloat16)
    pos_gaps = jax.random.randint(key_list[2], (SEQ_LEN,), 1, POS_GAP + 1)
    positions = (jnp.cumsum(pos_gaps) - pos_gaps[0]).astype(jnp.int32)

    def normal_weight(key_w, rows_in, cols_out):
        return (jax.random.normal(key_w, (rows_in, cols_out), jnp.float32) * rows_in ** -0.5).astype(jnp.bfloat16)

    def norm_param(key_w):
        return (0.3 * jax.random.normal(key_w, (D,), jnp.float32)).astype(jnp.bfloat16)

    return {
        "hidden": hidden,
        "positions": positions,
        "ln1_gain": norm_param(key_list[3]),
        "ln1_bias": norm_param(key_list[4]),
        "w_q": normal_weight(key_list[5], D, HEADS * HEAD),
        "w_k": normal_weight(key_list[6], D, KV_HEADS * HEAD),
        "w_v": normal_weight(key_list[7], D, KV_HEADS * HEAD),
        "w_o": normal_weight(key_list[8], HEADS * HEAD, D),
        "ln2_gain": norm_param(key_list[9]),
        "ln2_bias": norm_param(key_list[10]),
        "w_up": normal_weight(key_list[11], D, FF),
        "w_down": normal_weight(key_list[12], FF, D),
    }


def layer_norm_1p(in_rows, ln_gain, ln_bias):
    rows_f32 = in_rows.astype(jnp.float32)
    row_mean = jnp.mean(rows_f32, axis=-1, keepdims=True)
    centered = rows_f32 - row_mean
    row_var = jnp.mean(centered * centered, axis=-1, keepdims=True)
    scaled = centered * lax.rsqrt(row_var + LN_EPS)
    return (scaled * (1.0 + ln_gain.astype(jnp.float32)) + ln_bias.astype(jnp.float32)).astype(jnp.bfloat16)


def rope_tables(positions):
    rot_half = ROT_DIM // 2
    inv_freq = ROPE_BASE ** (-2.0 * jnp.arange(rot_half, dtype=jnp.float32) / ROT_DIM)
    pos_angle = positions.astype(jnp.float32)[:, None] * inv_freq[None, :]
    return jnp.cos(pos_angle), jnp.sin(pos_angle)


def apply_rope(heads_in, cos_b, sin_b):
    rot_half = ROT_DIM // 2
    heads_f32 = heads_in.astype(jnp.float32)
    lead_half = heads_f32[..., :rot_half]
    tail_half = heads_f32[..., rot_half:ROT_DIM]
    turned = jnp.concatenate([lead_half * cos_b - tail_half * sin_b, tail_half * cos_b + lead_half * sin_b], axis=-1)
    return jnp.concatenate([turned.astype(jnp.bfloat16), heads_in[..., ROT_DIM:]], axis=-1)


def reference(hidden, positions, ln1_gain, ln1_bias, w_q, w_k, w_v, w_o, ln2_gain, ln2_bias, w_up, w_down):
    q_group = HEADS // KV_HEADS
    cos_t, sin_t = rope_tables(positions)
    cos_b = cos_t[:, None, :]
    sin_b = sin_t[:, None, :]
    causal = jnp.arange(SEQ_LEN)[:, None] >= jnp.arange(SEQ_LEN)[None, :]

    def one_sample(x_rows):
        h_in = layer_norm_1p(x_rows, ln1_gain, ln1_bias)
        q_proj = jnp.dot(h_in, w_q, preferred_element_type=jnp.float32).astype(jnp.bfloat16).reshape(SEQ_LEN, HEADS, HEAD)
        k_proj = jnp.dot(h_in, w_k, preferred_element_type=jnp.float32).astype(jnp.bfloat16).reshape(SEQ_LEN, KV_HEADS, HEAD)
        v_proj = jnp.dot(h_in, w_v, preferred_element_type=jnp.float32).astype(jnp.bfloat16).reshape(SEQ_LEN, KV_HEADS, HEAD)
        q_proj = apply_rope(q_proj, cos_b, sin_b)
        k_proj = apply_rope(k_proj, cos_b, sin_b)
        k_full = jnp.repeat(k_proj, q_group, axis=1)
        v_full = jnp.repeat(v_proj, q_group, axis=1)
        scores = jnp.einsum("qhd,khd->hqk", q_proj.astype(jnp.float32), k_full.astype(jnp.float32)) * HEAD ** -0.5
        scores = jnp.where(causal[None, :, :], scores, -1e30)
        attn_prob = jax.nn.softmax(scores, axis=-1).astype(jnp.bfloat16)
        attn_out = jnp.einsum("hqk,khd->qhd", attn_prob.astype(jnp.float32), v_full.astype(jnp.float32)).astype(jnp.bfloat16)
        head_norm = jnp.sqrt(jnp.sum(jnp.square(attn_out.astype(jnp.float32)), axis=-1))
        o_sum = jnp.dot(attn_out.reshape(SEQ_LEN, HEADS * HEAD), w_o, preferred_element_type=jnp.float32)
        x_mid = (x_rows.astype(jnp.float32) + o_sum).astype(jnp.bfloat16)
        h_mid = layer_norm_1p(x_mid, ln2_gain, ln2_bias)
        mlp_act = jnp.square(jax.nn.relu(jnp.dot(h_mid, w_up, preferred_element_type=jnp.float32)))
        mlp_sum = jnp.dot(mlp_act.astype(jnp.bfloat16), w_down, preferred_element_type=jnp.float32)
        out_rows = (x_mid.astype(jnp.float32) + mlp_sum).astype(jnp.bfloat16)
        sample_means = (
            jnp.mean(mlp_act, axis=0),
            jnp.mean(head_norm, axis=0),
            jnp.mean(h_in.astype(jnp.float32), axis=0),
            jnp.mean(h_mid.astype(jnp.float32), axis=0),
        )
        return out_rows, sample_means

    out_hidden, mean_tuple = lax.map(one_sample, hidden)
    act_mean, head_mean, ln1_mean, ln2_mean = mean_tuple
    f_neuron = jnp.sqrt(jnp.sum(jnp.square(act_mean), axis=0))
    f_head = jnp.sqrt(jnp.sum(jnp.square(head_mean), axis=0))
    f_embed = jnp.sqrt(jnp.sum(jnp.square(ln1_mean), axis=0) + jnp.sum(jnp.square(ln2_mean), axis=0))
    return out_hidden, f_neuron, f_head, f_embed
```

```python
import functools

import jax
import jax.numpy as jnp
from jax import lax
from jax.experimental import pallas as pl
from jax.experimental.pallas import tpu as pltpu
from jax.sharding import PartitionSpec as P

HEAD_DIM = 128
ROT_DIM = 64
ROPE_BASE = 10000.0
LN_EPS = 1e-5
TILE = 512
NSLOT = 3
MESH = pl.DeviceIdType.MESH

UNITS = (
    ("rs1", 0), ("rs1", 1), ("ag1", 0), ("rs1", 2), ("ag1", 1), ("rs1", 3), ("rs2", 0), ("ag1", 2),
    ("rs2", 1), ("ag1", 3), ("ag2", 0), ("rs2", 2), ("ag2", 1), ("rs2", 3), ("ag2", 2), ("ag2", 3),
)
HEAD_PIECES = (("o", 0), ("o", 1))
SLOT_PIECES = {
    0: (("o", 2),), 2: (("o", 3),), 3: (("up", 0),), 4: (("dn", 0),), 5: (("up", 1),), 6: (("dn", 1),),
    8: (("up", 2),), 9: (("dn", 2),), 10: (("up", 3),), 11: (("dn", 3),),
}


def layer_norm_1p(in_rows, ln_gain, ln_bias):
    rows_f32 = in_rows.astype(jnp.float32)
    row_mean = jnp.mean(rows_f32, axis=-1, keepdims=True)
    centered = rows_f32 - row_mean
    row_var = jnp.mean(centered * centered, axis=-1, keepdims=True)
    scaled = centered * lax.rsqrt(row_var + LN_EPS)
    return (scaled * (1.0 + ln_gain.astype(jnp.float32)) + ln_bias.astype(jnp.float32)).astype(jnp.bfloat16)


def rope_tables(positions):
    rot_half = ROT_DIM // 2
    inv_freq = ROPE_BASE ** (-2.0 * jnp.arange(rot_half, dtype=jnp.float32) / ROT_DIM)
    pos_angle = positions.astype(jnp.float32)[:, None] * inv_freq[None, :]
    return jnp.cos(pos_angle), jnp.sin(pos_angle)


def apply_rope(heads_in, cos_b, sin_b):
    rot_half = ROT_DIM // 2
    heads_f32 = heads_in.astype(jnp.float32)
    lead_half = heads_f32[..., :rot_half]
    tail_half = heads_f32[..., rot_half:ROT_DIM]
    turned = jnp.concatenate([lead_half * cos_b - tail_half * sin_b, tail_half * cos_b + lead_half * sin_b], axis=-1)
    return jnp.concatenate([turned.astype(jnp.bfloat16), heads_in[..., ROT_DIM:]], axis=-1)


def attention_block(h_in, positions, w_q, w_k, w_v):
    n_batch = h_in.shape[0]
    n_seq = h_in.shape[1]
    kv_heads = w_k.shape[1] // HEAD_DIM
    q_group = w_q.shape[1] // w_k.shape[1]
    cos_t, sin_t = rope_tables(positions)
    q_proj = jnp.einsum("bsd,dn->bsn", h_in, w_q, preferred_element_type=jnp.float32).astype(jnp.bfloat16)
    q_proj = q_proj.reshape(n_batch, n_seq, kv_heads, q_group, HEAD_DIM)
    k_proj = jnp.einsum("bsd,dn->bsn", h_in, w_k, preferred_element_type=jnp.float32).astype(jnp.bfloat16)
    k_proj = k_proj.reshape(n_batch, n_seq, kv_heads, HEAD_DIM)
    v_proj = jnp.einsum("bsd,dn->bsn", h_in, w_v, preferred_element_type=jnp.float32).astype(jnp.bfloat16)
    v_proj = v_proj.reshape(n_batch, n_seq, kv_heads, HEAD_DIM)
    q_proj = apply_rope(q_proj, cos_t[None, :, None, None, :], sin_t[None, :, None, None, :])
    k_proj = apply_rope(k_proj, cos_t[None, :, None, :], sin_t[None, :, None, :])
    scores = jnp.einsum("bqkgd,bskd->bkgqs", q_proj, k_proj, preferred_element_type=jnp.float32) * HEAD_DIM ** -0.5
    causal = jnp.arange(n_seq)[:, None] >= jnp.arange(n_seq)[None, :]
    scores = jnp.where(causal, scores, -1e30)
    attn_prob = jax.nn.softmax(scores, axis=-1).astype(jnp.bfloat16)
    return jnp.einsum("bkgqs,bskd->bqkgd", attn_prob, v_proj, preferred_element_type=jnp.float32).astype(jnp.bfloat16)


def layer_kernel(
    n_tp, n_dp, attn_ref, esq_ref, head_ref, gain_ref, bias_ref, hid_ref, wo_ref, wup_ref, wdn_ref,
    y_ref, score_ref,
    wbuf, part, rbuf, gath, hmid, act, xmid, ystage, nsq, esq, sbuf, xbuf,
    wsem, ssem, rsem, hsem, ysem, xssem, xrsem,
):
    me = lax.axis_index("tp")
    my_dp = lax.axis_index("dp")
    right = lax.rem(me + 1, n_tp)
    left = lax.rem(me + n_tp - 1, n_tp)
    opp = lax.rem(me + 2, n_tp)
    n_seq = part.shape[1]
    width = part.shape[2]
    blk = n_seq // n_tp
    half = blk // 2
    k_o = wo_ref.shape[0]
    partners = []
    step = 1
    while step < n_dp:
        bit = lax.rem(my_dp // step, 2)
        partners.append(my_dp + step - 2 * step * bit)
        step *= 2

    def half_rows(owner, which):
        return pl.ds(pl.multiple_of(owner * blk + which * half, half), half)

    pieces = list(HEAD_PIECES)
    for k in range(len(UNITS)):
        pieces.extend(SLOT_PIECES.get(k, ()))

    def n_tiles(kind):
        return (wup_ref if kind == "up" else wdn_ref).shape[1] // TILE

    bases = {}
    base = 0
    for piece in pieces:
        bases[piece] = base
        base += n_tiles(piece[0])

    def tile_copy(piece, i):
        slot = lax.rem(bases[piece] + i, NSLOT)
        cols = pl.ds(pl.multiple_of(i * TILE, TILE), TILE)
        if piece[0] == "o":
            return pltpu.make_async_copy(wo_ref.at[:, cols], wbuf.at[slot, pl.ds(0, k_o), :], wsem.at[slot])
        src = wup_ref if piece[0] == "up" else wdn_ref
        return pltpu.make_async_copy(src.at[:, cols], wbuf.at[slot], wsem.at[slot])

    def prefetch(piece):
        for i in range(NSLOT - 1):
            tile_copy(piece, i).start()

    def run_piece(piece):
        kind, seq = piece
        tiles = n_tiles(kind)

        def body(i, carry):
            tile_copy(piece, i).wait()

            @pl.when(i + NSLOT - 1 < tiles)
            def _():
                tile_copy(piece, i + NSLOT - 1).start()

            slot = lax.rem(bases[piece] + i, NSLOT)
            cols = pl.ds(pl.multiple_of(i * TILE, TILE), TILE)
            if kind == "o":
                part[seq % 3, :, cols] = jnp.dot(
                    attn_ref[seq], wbuf[slot, pl.ds(0, k_o), :], preferred_element_type=jnp.float32
                )
            elif kind == "up":
                up = jnp.maximum(jnp.dot(hmid[...], wbuf[slot], preferred_element_type=jnp.float32), 0.0)
                sq = up * up
                mean = jnp.sum(sq, axis=0, keepdims=True) * (1.0 / n_seq)
                nsq[:, cols] += mean * mean
                act[:, cols] = sq.astype(jnp.bfloat16)
            else:
                part[(4 + seq) % 3, :, cols] = jnp.dot(act[...], wbuf[slot], preferred_element_type=jnp.float32)
            return carry

        lax.fori_loop(0, tiles, body, 0)
        after = pieces.index(piece) + 1
        if after < len(pieces):
            prefetch(pieces[after])

    def remote(src, dst, k, direction, j):
        return pltpu.make_async_remote_copy(
            src_ref=src, dst_ref=dst, send_sem=ssem.at[k, direction, j], recv_sem=rsem.at[k, direction, j],
            device_id={"tp": right if direction == 0 else left}, device_id_type=MESH,
        )

    def unit_copies(k):
        kind, seq = UNITS[k]
        ix = seq if kind[2] == "1" else 4 + seq
        if kind[:2] == "rs":
            p = ix % 3
            routes = (
                ((opp, 0), (right, 1), (right, 0)),
                ((opp, 1), (left, 0), (left, 1)),
            )
            return [
                [
                    remote(part.at[p, half_rows(*routes[d][j]), :], rbuf.at[ix, d, j], k, d, j)
                    for j in range(3)
                ]
                for d in range(2)
            ]
        routes = (
            ((me, 0), (me, 1), (left, 0)),
            ((me, 1), (me, 0), (right, 1)),
        )
        return [
            [
                remote(
                    gath.at[ix, half_rows(*routes[d][j]), :], gath.at[ix, half_rows(*routes[d][j]), :], k, d, j
                )
                for j in range(3)
            ]
            for d in range(2)
        ]

    copies = [unit_copies(k) for k in range(len(UNITS))]

    def begin(k):
        for j in range(2):
            for d in range(2):
                copies[k][d][j].start()

    def middle(k):
        kind, seq = UNITS[k]
        ix = seq if kind[2] == "1" else 4 + seq
        for d in range(2):
            copies[k][d][0].wait_recv()
            if kind[:2] == "rs":
                rows = half_rows(right if d == 0 else left, d)
                part[ix % 3, rows, :] = part[ix % 3, rows, :] + rbuf[ix, d, 0]
            copies[k][d][2].start()

    def norm_rows(rows):
        mean = jnp.sum(rows, axis=-1, keepdims=True) * (1.0 / width)
        centered = rows - mean
        var = jnp.sum(centered * centered, axis=-1, keepdims=True) * (1.0 / width)
        scaled = centered * lax.rsqrt(var + LN_EPS)
        out = scaled * (1.0 + gain_ref[...].astype(jnp.float32)) + bias_ref[...].astype(jnp.float32)
        return out.astype(jnp.bfloat16).astype(jnp.float32)

    def finish(k):
        kind, seq = UNITS[k]
        ix = seq if kind[2] == "1" else 4 + seq
        for d in range(2):
            for j in (1, 2):
                copies[k][d][j].wait_recv()
        if kind[:2] == "rs":
            for w in range(2):
                rows = half_rows(me, w)
                total = part[ix % 3, rows, :] + rbuf[ix, w, 2] + rbuf[ix, 1 - w, 1]
                mine = pl.ds(w * half, half)
                mid = (xmid[seq, mine, :].astype(jnp.float32) + total).astype(jnp.bfloat16)
                if kind == "rs1":
                    xmid[seq, mine, :] = mid
                    gath[ix, rows, :] = norm_rows(mid.astype(jnp.float32))
                else:
                    gath[ix, rows, :] = mid.astype(jnp.float32)
        elif kind == "ag1":
            def cast(i, carry):
                cols = pl.ds(pl.multiple_of(i * TILE, TILE), TILE)
                got = gath[ix, :, cols]
                mean = jnp.sum(got, axis=0, keepdims=True) * (1.0 / n_seq)
                esq[:, cols] += mean * mean
                hmid[:, cols] = got.astype(jnp.bfloat16)
                return carry

            lax.fori_loop(0, width // TILE, cast, 0)
        else:
            if seq >= 2:
                y_copy(seq - 2).wait()

            def store(i, carry):
                cols = pl.ds(pl.multiple_of(i * TILE, TILE), TILE)
                ystage[seq % 2, :, cols] = gath[ix, :, cols].astype(jnp.bfloat16)
                return carry

            lax.fori_loop(0, width // TILE, store, 0)
            y_copy(seq).start()
        for d in range(2):
            for j in range(3):
                copies[k][d][j].wait_send()

    def y_copy(seq):
        return pltpu.make_async_copy(ystage.at[seq % 2], y_ref.at[seq], ysem.at[seq % 2])

    def score_copy(i):
        return pltpu.make_async_remote_copy(
            src_ref=sbuf.at[i], dst_ref=xbuf.at[i], send_sem=xssem.at[i], recv_sem=xrsem.at[i],
            device_id={"dp": partners[i]}, device_id_type=MESH,
        )

    def score_begin():
        per = width // 8
        fper = nsq.shape[1] // 8
        for r in range(8):
            sbuf[0, r : r + 1, 0:fper] = nsq[:, r * fper : (r + 1) * fper]
            sbuf[0, r : r + 1, fper : fper + per] = esq[:, r * per : (r + 1) * per]
            sbuf[0, r : r + 1, fper + per : fper + per + 128] = head_ref[...]
        score_copy(0).start()

    def score_step(i):
        score_copy(i).wait()
        sbuf[i + 1] = sbuf[i] + xbuf[i]
        if i + 1 < len(partners):
            score_copy(i + 1).start()

    prefetch(pieces[0])
    hid_copies = [
        pltpu.make_async_copy(
            hid_ref.at[seq, pl.ds(pl.multiple_of(me * blk, blk), blk), :], xmid.at[seq], hsem.at[seq]
        )
        for seq in range(hid_ref.shape[0])
    ]
    for copy in hid_copies:
        copy.start()
    nsq[...] = jnp.zeros_like(nsq)
    esq[...] = esq_ref[...]

    barrier = pltpu.get_barrier_semaphore()
    for t in (left, right):
        pl.semaphore_signal(barrier, inc=1, device_id={"tp": t}, device_id_type=MESH)
    for other in partners:
        pl.semaphore_signal(barrier, inc=1, device_id={"dp": other}, device_id_type=MESH)
    pl.semaphore_wait(barrier, 2 + len(partners))

    run_piece(HEAD_PIECES[0])
    begin(0)
    for copy in hid_copies:
        copy.wait()
    for piece in HEAD_PIECES[1:]:
        run_piece(piece)
    last = len(UNITS) - 1
    for k in range(len(UNITS)):
        if k > 0:
            finish(k - 1)
        if k < last:
            begin(k + 1)
        middle(k)
        for piece in SLOT_PIECES.get(k, ()):
            run_piece(piece)
        if k == 10:
            score_begin()
        elif k > 10:
            score_step(k - 11)
    finish(last)
    for i in range(last - 10, len(partners)):
        score_step(i)
    score_ref[...] = sbuf[len(partners)]
    for seq in (2, 3):
        y_copy(seq).wait()


def solution(mesh):
    n_tp = mesh.shape["tp"]
    n_dp = mesh.shape["dp"]

    def local_layer(hidden, positions, ln1_gain, ln1_bias, w_q, w_k, w_v, w_o, ln2_gain, ln2_bias, w_up, w_down):
        n_batch, n_seq, width = hidden.shape
        ff_local = w_up.shape[1]
        h_in = layer_norm_1p(hidden, ln1_gain, ln1_bias)
        attn_out = attention_block(h_in, positions, w_q, w_k, w_v)
        head_norm = jnp.sqrt(jnp.sum(jnp.square(attn_out.astype(jnp.float32)), axis=-1)).reshape(n_batch, n_seq, -1)
        head_sq = jnp.sum(jnp.square(jnp.mean(head_norm, axis=1)), axis=0)
        heads_local = head_sq.shape[0]
        ln1_sq = jnp.sum(jnp.square(jnp.mean(h_in, axis=1, dtype=jnp.float32)), axis=0)
        head_row = jnp.pad(head_sq, (0, 128 - heads_local)).reshape(1, 128)
        score_cols = ff_local // 8 + width // 8 + 128
        n_stage = n_dp.bit_length() - 1
        blk = n_seq // n_tp
        any_spec = pl.BlockSpec(memory_space=pl.ANY)
        vmem_spec = pl.BlockSpec(memory_space=pltpu.VMEM)
        n_units = len(UNITS)
        y, score = pl.pallas_call(
            functools.partial(layer_kernel, n_tp, n_dp),
            out_shape=(
                jax.ShapeDtypeStruct(hidden.shape, jnp.bfloat16),
                jax.ShapeDtypeStruct((8, score_cols), jnp.float32),
            ),
            in_specs=[vmem_spec] * 5 + [any_spec] * 4,
            out_specs=(any_spec, vmem_spec),
            scratch_shapes=[
                pltpu.VMEM((NSLOT, width, TILE), jnp.bfloat16),
                pltpu.VMEM((3, n_seq, width), jnp.float32),
                pltpu.VMEM((2 * n_batch, 2, 3, blk // 2, width), jnp.float32),
                pltpu.VMEM((2 * n_batch, n_seq, width), jnp.float32),
                pltpu.VMEM((n_seq, width), jnp.bfloat16),
                pltpu.VMEM((n_seq, ff_local), jnp.bfloat16),
                pltpu.VMEM((n_batch, blk, width), jnp.bfloat16),
                pltpu.VMEM((2, n_seq, width), jnp.bfloat16),
                pltpu.VMEM((1, ff_local), jnp.float32),
                pltpu.VMEM((1, width), jnp.float32),
                pltpu.VMEM((n_stage + 1, 8, score_cols), jnp.float32),
                pltpu.VMEM((n_stage, 8, score_cols), jnp.float32),
                pltpu.SemaphoreType.DMA((NSLOT,)),
                pltpu.SemaphoreType.DMA((n_units, 2, 3)),
                pltpu.SemaphoreType.DMA((n_units, 2, 3)),
                pltpu.SemaphoreType.DMA((n_batch,)),
                pltpu.SemaphoreType.DMA((2,)),
                pltpu.SemaphoreType.DMA((n_stage,)),
                pltpu.SemaphoreType.DMA((n_stage,)),
            ],
            compiler_params=pltpu.CompilerParams(
                collective_id=0, has_side_effects=True, vmem_limit_bytes=66_000_000
            ),
            name="layer",
        )(
            attn_out.reshape(n_batch, n_seq, -1), ln1_sq.reshape(1, width), head_row,
            ln2_gain.reshape(1, width), ln2_bias.reshape(1, width), hidden, w_o, w_up, w_down,
        )
        roots = jnp.sqrt(score)
        f_neuron = roots[:, : ff_local // 8].reshape(ff_local)
        f_embed = roots[:, ff_local // 8 : ff_local // 8 + width // 8].reshape(width)
        f_head = roots[0, ff_local // 8 + width // 8 :][:heads_local]
        return y, f_neuron, f_head, f_embed

    weight_col = P(None, "tp")
    weight_row = P("tp", None)
    return jax.shard_map(
        local_layer,
        mesh=mesh,
        in_specs=(P("dp"), P(), P(), P(), weight_col, weight_col, weight_col, weight_row, P(), P(), weight_col, weight_row),
        out_specs=(P("dp"), P("tp"), P("tp"), P()),
        check_vma=False,
    )
```

```python
import functools

import jax
import jax.numpy as jnp
from jax import lax
from jax.experimental import pallas as pl
from jax.experimental.pallas import tpu as pltpu
from jax.sharding import PartitionSpec as P

HEAD_DIM = 128
ROT_DIM = 64
ROPE_BASE = 10000.0
LN_EPS = 1e-5
TILE = 512
NSLOT = 3
MESH = pl.DeviceIdType.MESH

UNITS = (
    ("rs1", 0), ("rs1", 1), ("ag1", 0), ("rs1", 2), ("ag1", 1), ("rs1", 3), ("rs2", 0), ("ag1", 2),
    ("rs2", 1), ("ag1", 3), ("ag2", 0), ("rs2", 2), ("ag2", 1), ("rs2", 3), ("ag2", 2), ("ag2", 3),
)
HEAD_PIECES = (("qkv", 0), ("o", 0), ("qkv", 1), ("o", 1))
SLOT_PIECES = {
    0: (("qkv", 2), ("o", 2)), 2: (("qkv", 3), ("o", 3)), 3: (("up", 0),), 4: (("dn", 0),), 5: (("up", 1),), 6: (("dn", 1),),
    8: (("up", 2),), 9: (("dn", 2),), 10: (("up", 3),), 11: (("dn", 3),),
}


def rope_lanes(positions):
    half_rot = ROT_DIM // 2
    lane = jnp.arange(HEAD_DIM)
    inv_freq = ROPE_BASE ** (-2.0 * (lane % half_rot).astype(jnp.float32) / ROT_DIM)
    angle = positions.astype(jnp.float32)[:, None] * inv_freq[None, :]
    sign = jnp.where(lane < half_rot, -1.0, 1.0)
    cos_l = jnp.where(lane < ROT_DIM, jnp.cos(angle), 1.0)
    sin_l = jnp.where(lane < ROT_DIM, sign * jnp.sin(angle), 0.0)
    return cos_l, sin_l


def layer_kernel(
    n_tp, n_dp, cos_ref, sin_ref, norm_ref, hid_ref, wq_ref, wk_ref, wv_ref, wo_ref, wup_ref, wdn_ref,
    y_ref, score_ref,
    wbuf, part, rbuf, gath, hmid, act, xmid, ystage, nsq, esq, hsq, sbuf, xbuf,
    wsem, vsem, ssem, rsem, hsem, xsem, ysem, xssem, xrsem,
):
    me = lax.axis_index("tp")
    my_dp = lax.axis_index("dp")
    right = lax.rem(me + 1, n_tp)
    left = lax.rem(me + n_tp - 1, n_tp)
    opp = lax.rem(me + 2, n_tp)
    n_seq = part.shape[1]
    width = part.shape[2]
    blk = n_seq // n_tp
    half = blk // 2
    k_o = wo_ref.shape[0]
    partners = []
    step = 1
    while step < n_dp:
        bit = lax.rem(my_dp // step, 2)
        partners.append(my_dp + step - 2 * step * bit)
        step *= 2

    def half_rows(owner, which):
        return pl.ds(pl.multiple_of(owner * blk + which * half, half), half)

    pieces = list(HEAD_PIECES)
    for k in range(len(UNITS)):
        pieces.extend(SLOT_PIECES.get(k, ()))

    n_q = wq_ref.shape[1]
    n_kv = wk_ref.shape[1]
    n_qkv = n_q + 2 * n_kv
    q_tiles = n_q // TILE
    group = n_q // n_kv

    def n_tiles(kind):
        if kind == "qkv":
            return q_tiles + 1
        return (wup_ref if kind == "up" else wdn_ref).shape[1] // TILE

    bases = {}
    base = 0
    for piece in pieces:
        bases[piece] = base
        base += n_tiles(piece[0])

    def tile_slot(piece, i):
        return lax.rem(bases[piece] + i, NSLOT)

    def tile_copy(piece, i):
        slot = tile_slot(piece, i)
        cols = pl.ds(pl.multiple_of(i * TILE, TILE), TILE)
        if piece[0] == "o":
            return pltpu.make_async_copy(wo_ref.at[:, cols], wbuf.at[slot, pl.ds(0, k_o), :], wsem.at[slot])
        src = {"qkv": wq_ref, "up": wup_ref, "dn": wdn_ref}[piece[0]]
        return pltpu.make_async_copy(src.at[:, cols], wbuf.at[slot], wsem.at[slot])

    def kv_copies(piece):
        slot = tile_slot(piece, q_tiles)
        return (
            pltpu.make_async_copy(wk_ref, wbuf.at[slot, :, pl.ds(0, n_kv)], wsem.at[slot]),
            pltpu.make_async_copy(wv_ref, wbuf.at[slot, :, pl.ds(n_kv, n_kv)], vsem),
        )

    def start_tile(piece, i):
        if piece[0] != "qkv":
            tile_copy(piece, i).start()
            return

        @pl.when(i < q_tiles)
        def _():
            tile_copy(piece, i).start()

        @pl.when(i == q_tiles)
        def _():
            for copy in kv_copies(piece):
                copy.start()

    def prefetch(piece):
        for i in range(NSLOT - 1):
            tile_copy(piece, i).start()

    def norm_rows(rows, which):
        mean = jnp.sum(rows, axis=-1, keepdims=True) * (1.0 / width)
        centered = rows - mean
        var = jnp.sum(centered * centered, axis=-1, keepdims=True) * (1.0 / width)
        scaled = centered * lax.rsqrt(var + LN_EPS)
        out = scaled * norm_ref[pl.ds(2 * which, 1), :] + norm_ref[pl.ds(2 * which + 1, 1), :]
        return out.astype(jnp.bfloat16)

    def seq_copy(seq):
        return pltpu.make_async_copy(hid_ref.at[seq], ystage.at[seq % 2], xsem.at[seq % 2])

    def first_norm(seq):
        seq_copy(seq).wait()

        def rows_body(i, carry):
            rows = pl.ds(pl.multiple_of(i * 16, 16), 16)
            hmid[rows, :] = norm_rows(ystage[seq % 2, rows, :].astype(jnp.float32), 0)
            return carry

        lax.fori_loop(0, n_seq // 16, rows_body, 0)
        if seq + 2 < hid_ref.shape[0]:
            seq_copy(seq + 2).start()

    def first_means():
        def cols_body(i, carry):
            cols = pl.ds(pl.multiple_of(i * TILE, TILE), TILE)
            mean = jnp.sum(hmid[:, cols].astype(jnp.float32), axis=0, keepdims=True) * (1.0 / n_seq)
            esq[:, cols] += mean * mean
            return carry

        lax.fori_loop(0, width // TILE, cols_body, 0)

    def rotate(raw, lane):
        rot_half = ROT_DIM // 2
        val = raw.astype(jnp.float32)
        ahead = pltpu.roll(val, HEAD_DIM - rot_half, 1)
        behind = pltpu.roll(val, rot_half, 1)
        partner = jnp.where(lane < rot_half, ahead, behind)
        return (val * cos_ref[...] + partner * sin_ref[...]).astype(jnp.bfloat16)

    def attend():
        lane = lax.broadcasted_iota(jnp.int32, (n_seq, HEAD_DIM), 1)
        row = lax.broadcasted_iota(jnp.int32, (n_seq, n_seq), 0)
        col = lax.broadcasted_iota(jnp.int32, (n_seq, n_seq), 1)
        lane_row = lax.broadcasted_iota(jnp.int32, (1, HEAD_DIM), 1)

        def group_body(g, carry):
            def head_cols(start):
                return pl.ds(pl.multiple_of(start, HEAD_DIM), HEAD_DIM)

            keys = rotate(act[:, head_cols(n_q + g * HEAD_DIM)], lane)
            vals = act[:, head_cols(n_q + n_kv + g * HEAD_DIM)]
            for i in range(group):
                head = g * group + i
                query = rotate(act[:, head_cols(head * HEAD_DIM)], lane)
                scores = lax.dot_general(
                    query, keys, (((1,), (1,)), ((), ())), preferred_element_type=jnp.float32
                ) * HEAD_DIM ** -0.5
                scores = jnp.where(row >= col, scores, -1e30)
                top = jnp.max(scores, axis=-1, keepdims=True)
                exps = jnp.exp(scores - top)
                prob = (exps * (1.0 / jnp.sum(exps, axis=-1, keepdims=True))).astype(jnp.bfloat16)
                out = jnp.dot(prob, vals, preferred_element_type=jnp.float32).astype(jnp.bfloat16)
                act[:, head_cols(n_qkv + head * HEAD_DIM)] = out
                out32 = out.astype(jnp.float32)
                norm = jnp.sqrt(jnp.sum(out32 * out32, axis=-1, keepdims=True))
                mean = jnp.sum(norm, axis=0, keepdims=True) * (1.0 / n_seq)
                hsq[...] += jnp.where(lane_row == head, mean * mean, 0.0)
            return carry

        lax.fori_loop(0, n_kv // HEAD_DIM, group_body, 0)

    def run_piece(piece):
        kind, seq = piece
        tiles = n_tiles(kind)
        if kind == "qkv":
            first_norm(seq)

        def body(i, carry):
            tile_copy(piece, i).wait()

            @pl.when(i + NSLOT - 1 < tiles)
            def _():
                start_tile(piece, i + NSLOT - 1)

            slot = tile_slot(piece, i)
            cols = pl.ds(pl.multiple_of(i * TILE, TILE), TILE)
            if kind == "qkv":
                act[:, cols] = jnp.dot(hmid[...], wbuf[slot], preferred_element_type=jnp.float32).astype(jnp.bfloat16)
            elif kind == "o":
                part[seq % 3, :, cols] = jnp.dot(
                    act[:, pl.ds(n_qkv, n_q)], wbuf[slot, pl.ds(0, k_o), :], preferred_element_type=jnp.float32
                )
            elif kind == "up":
                up = jnp.maximum(jnp.dot(hmid[...], wbuf[slot], preferred_element_type=jnp.float32), 0.0)
                sq = up * up
                mean = jnp.sum(sq, axis=0, keepdims=True) * (1.0 / n_seq)
                nsq[:, cols] += mean * mean
                act[:, cols] = sq.astype(jnp.bfloat16)
            else:
                part[(4 + seq) % 3, :, cols] = jnp.dot(act[...], wbuf[slot], preferred_element_type=jnp.float32)
            return carry

        lax.fori_loop(0, q_tiles if kind == "qkv" else tiles, body, 0)
        if kind == "qkv":
            for copy in kv_copies(piece):
                copy.wait()
            act[:, pl.ds(n_q, 2 * n_kv)] = jnp.dot(
                hmid[...], wbuf[tile_slot(piece, q_tiles)], preferred_element_type=jnp.float32
            ).astype(jnp.bfloat16)
        after = pieces.index(piece) + 1
        if after < len(pieces):
            prefetch(pieces[after])
        if kind == "qkv":
            attend()

    def remote(src, dst, k, direction, j):
        return pltpu.make_async_remote_copy(
            src_ref=src, dst_ref=dst, send_sem=ssem.at[k, direction, j], recv_sem=rsem.at[k, direction, j],
            device_id={"tp": right if direction == 0 else left}, device_id_type=MESH,
        )

    def unit_copies(k):
        kind, seq = UNITS[k]
        ix = seq if kind[2] == "1" else 4 + seq
        if kind[:2] == "rs":
            p = ix % 3
            routes = (
                ((opp, 0), (right, 1), (right, 0)),
                ((opp, 1), (left, 0), (left, 1)),
            )
            return [
                [
                    remote(part.at[p, half_rows(*routes[d][j]), :], rbuf.at[ix, d, j], k, d, j)
                    for j in range(3)
                ]
                for d in range(2)
            ]
        routes = (
            ((me, 0), (me, 1), (left, 0)),
            ((me, 1), (me, 0), (right, 1)),
        )
        return [
            [
                remote(
                    gath.at[ix, half_rows(*routes[d][j]), :], gath.at[ix, half_rows(*routes[d][j]), :], k, d, j
                )
                for j in range(3)
            ]
            for d in range(2)
        ]

    copies = [unit_copies(k) for k in range(len(UNITS))]

    def begin(k):
        for j in range(2):
            for d in range(2):
                copies[k][d][j].start()

    def middle(k):
        kind, seq = UNITS[k]
        ix = seq if kind[2] == "1" else 4 + seq
        for d in range(2):
            copies[k][d][0].wait_recv()
            if kind[:2] == "rs":
                rows = half_rows(right if d == 0 else left, d)
                part[ix % 3, rows, :] = part[ix % 3, rows, :] + rbuf[ix, d, 0]
            copies[k][d][2].start()

    def finish(k):
        kind, seq = UNITS[k]
        ix = seq if kind[2] == "1" else 4 + seq
        for d in range(2):
            for j in (1, 2):
                copies[k][d][j].wait_recv()
        if kind[:2] == "rs":
            for w in range(2):
                rows = half_rows(me, w)
                total = part[ix % 3, rows, :] + rbuf[ix, w, 2] + rbuf[ix, 1 - w, 1]
                mine = pl.ds(w * half, half)
                mid = (xmid[seq, mine, :].astype(jnp.float32) + total).astype(jnp.bfloat16)
                if kind == "rs1":
                    xmid[seq, mine, :] = mid
                    gath[ix, rows, :] = norm_rows(mid.astype(jnp.float32), 1).astype(jnp.float32)
                else:
                    gath[ix, rows, :] = mid.astype(jnp.float32)
        elif kind == "ag1":
            def cast(i, carry):
                cols = pl.ds(pl.multiple_of(i * TILE, TILE), TILE)
                got = gath[ix, :, cols]
                mean = jnp.sum(got, axis=0, keepdims=True) * (1.0 / n_seq)
                esq[:, cols] += mean * mean
                hmid[:, cols] = got.astype(jnp.bfloat16)
                return carry

            lax.fori_loop(0, width // TILE, cast, 0)
        else:
            if seq >= 2:
                y_copy(seq - 2).wait()

            def store(i, carry):
                cols = pl.ds(pl.multiple_of(i * TILE, TILE), TILE)
                ystage[seq % 2, :, cols] = gath[ix, :, cols].astype(jnp.bfloat16)
                return carry

            lax.fori_loop(0, width // TILE, store, 0)
            y_copy(seq).start()
        for d in range(2):
            for j in range(3):
                copies[k][d][j].wait_send()

    def y_copy(seq):
        return pltpu.make_async_copy(ystage.at[seq % 2], y_ref.at[seq], ysem.at[seq % 2])

    def score_copy(i):
        return pltpu.make_async_remote_copy(
            src_ref=sbuf.at[i], dst_ref=xbuf.at[i], send_sem=xssem.at[i], recv_sem=xrsem.at[i],
            device_id={"dp": partners[i]}, device_id_type=MESH,
        )

    def score_begin():
        n_rows, e_rows = nsq.shape[1] // 128, width // 128
        for r in range(n_rows):
            sbuf[0, r : r + 1, :] = nsq[:, r * 128 : (r + 1) * 128]
        for r in range(e_rows):
            sbuf[0, n_rows + r : n_rows + r + 1, :] = esq[:, r * 128 : (r + 1) * 128]
        sbuf[0, n_rows + e_rows :, :] = jnp.broadcast_to(hsq[...], (8, 128))
        score_copy(0).start()

    def score_step(i):
        score_copy(i).wait()
        sbuf[i + 1] = sbuf[i] + xbuf[i]
        if i + 1 < len(partners):
            score_copy(i + 1).start()

    seq_copy(0).start()
    prefetch(pieces[0])
    seq_copy(1).start()
    hid_copies = [
        pltpu.make_async_copy(
            hid_ref.at[seq, pl.ds(pl.multiple_of(me * blk, blk), blk), :], xmid.at[seq], hsem.at[seq]
        )
        for seq in range(hid_ref.shape[0])
    ]
    for copy in hid_copies:
        copy.start()
    nsq[...] = jnp.zeros_like(nsq)
    esq[...] = jnp.zeros_like(esq)
    hsq[...] = jnp.zeros_like(hsq)

    barrier = pltpu.get_barrier_semaphore()
    for t in (left, right):
        pl.semaphore_signal(barrier, inc=1, device_id={"tp": t}, device_id_type=MESH)
    for other in partners:
        pl.semaphore_signal(barrier, inc=1, device_id={"dp": other}, device_id_type=MESH)
    pl.semaphore_wait(barrier, 2 + len(partners))

    run_piece(HEAD_PIECES[0])
    run_piece(HEAD_PIECES[1])
    begin(0)
    first_means()
    for copy in hid_copies:
        copy.wait()
    for piece in HEAD_PIECES[2:]:
        run_piece(piece)
    first_means()
    last = len(UNITS) - 1
    for k in range(len(UNITS)):
        if k > 0:
            finish(k - 1)
        if k < last:
            begin(k + 1)
        middle(k)
        for piece in SLOT_PIECES.get(k, ()):
            run_piece(piece)
            if piece[0] == "o":
                first_means()
        if k == 10:
            score_begin()
        elif k > 10:
            score_step(k - 11)
    finish(last)
    for i in range(last - 10, len(partners)):
        score_step(i)
    score_ref[...] = jnp.sqrt(sbuf[len(partners)])
    for seq in (2, 3):
        y_copy(seq).wait()


def solution(mesh):
    n_tp = mesh.shape["tp"]
    n_dp = mesh.shape["dp"]

    def local_layer(hidden, positions, ln1_gain, ln1_bias, w_q, w_k, w_v, w_o, ln2_gain, ln2_bias, w_up, w_down):
        n_batch, n_seq, width = hidden.shape
        ff_local = w_up.shape[1]
        heads_local = w_q.shape[1] // HEAD_DIM
        cos_l, sin_l = rope_lanes(positions)
        norm_rows = jnp.stack([
            1.0 + ln1_gain.astype(jnp.float32), ln1_bias.astype(jnp.float32),
            1.0 + ln2_gain.astype(jnp.float32), ln2_bias.astype(jnp.float32),
        ])
        n_rows, e_rows = ff_local // 128, width // 128
        score_rows = n_rows + e_rows + 8
        n_stage = n_dp.bit_length() - 1
        blk = n_seq // n_tp
        any_spec = pl.BlockSpec(memory_space=pl.ANY)
        vmem_spec = pl.BlockSpec(memory_space=pltpu.VMEM)
        n_units = len(UNITS)
        y, score = pl.pallas_call(
            functools.partial(layer_kernel, n_tp, n_dp),
            out_shape=(
                jax.ShapeDtypeStruct(hidden.shape, jnp.bfloat16),
                jax.ShapeDtypeStruct((score_rows, 128), jnp.float32),
            ),
            in_specs=[vmem_spec] * 3 + [any_spec] * 7,
            out_specs=(any_spec, vmem_spec),
            scratch_shapes=[
                pltpu.VMEM((NSLOT, width, TILE), jnp.bfloat16),
                pltpu.VMEM((3, n_seq, width), jnp.float32),
                pltpu.VMEM((2 * n_batch, 2, 3, blk // 2, width), jnp.float32),
                pltpu.VMEM((2 * n_batch, n_seq, width), jnp.float32),
                pltpu.VMEM((n_seq, width), jnp.bfloat16),
                pltpu.VMEM((n_seq, ff_local), jnp.bfloat16),
                pltpu.VMEM((n_batch, blk, width), jnp.bfloat16),
                pltpu.VMEM((2, n_seq, width), jnp.bfloat16),
                pltpu.VMEM((1, ff_local), jnp.float32),
                pltpu.VMEM((1, width), jnp.float32),
                pltpu.VMEM((1, 128), jnp.float32),
                pltpu.VMEM((n_stage + 1, score_rows, 128), jnp.float32),
                pltpu.VMEM((n_stage, score_rows, 128), jnp.float32),
                pltpu.SemaphoreType.DMA((NSLOT,)),
                pltpu.SemaphoreType.DMA,
                pltpu.SemaphoreType.DMA((n_units, 2, 3)),
                pltpu.SemaphoreType.DMA((n_units, 2, 3)),
                pltpu.SemaphoreType.DMA((n_batch,)),
                pltpu.SemaphoreType.DMA((2,)),
                pltpu.SemaphoreType.DMA((2,)),
                pltpu.SemaphoreType.DMA((n_stage,)),
                pltpu.SemaphoreType.DMA((n_stage,)),
            ],
            compiler_params=pltpu.CompilerParams(
                collective_id=0, has_side_effects=True, vmem_limit_bytes=66_000_000
            ),
            name="layer",
        )(cos_l, sin_l, norm_rows, hidden, w_q, w_k, w_v, w_o, w_up, w_down)
        f_neuron = score[:n_rows].reshape(ff_local)
        f_embed = score[n_rows : n_rows + e_rows].reshape(width)
        f_head = score[n_rows + e_rows, :heads_local]
        return y, f_neuron, f_head, f_embed

    weight_col = P(None, "tp")
    weight_row = P("tp", None)
    return jax.shard_map(
        local_layer,
        mesh=mesh,
        in_specs=(P("dp"), P(), P(), P(), weight_col, weight_col, weight_col, weight_row, P(), P(), weight_col, weight_row),
        out_specs=(P("dp"), P("tp"), P("tp"), P()),
        check_vma=False,
    )
```

```python
import functools

import jax
import jax.numpy as jnp
import numpy as np
from jax import lax
from jax.experimental import pallas as pl
from jax.experimental.pallas import tpu as pltpu
from jax.sharding import PartitionSpec as P

HEAD_DIM = 128
ROT_DIM = 64
ROPE_BASE = 10000.0
LN_EPS = 1e-5
TILE = 512
NSLOT = 3
MESH = pl.DeviceIdType.MESH

PROGRAM = (
    ("qkv", 0, 0), ("att", 0, 0), ("o", 0, 0), ("o", 0, 1), ("begin", "rs1", 0), ("mean", 0, 0), ("qkv", 1, 0),
    ("att", 1, 0), ("mid", "rs1", 0), ("o", 1, 0), ("o", 1, 1), ("begin", "rs1", 1), ("mean", 1, 0), ("qkv", 2, 0),
    ("fin", "rs1", 0), ("begin", "ag1", 0), ("att", 2, 0), ("mid", "rs1", 1), ("o", 2, 0), ("o", 2, 1),
    ("begin", "rs1", 2), ("mean", 2, 0), ("qkv", 3, 0), ("mid", "ag1", 0), ("att", 3, 0), ("o", 3, 0),
    ("fin", "rs1", 1), ("begin", "ag1", 1), ("o", 3, 1), ("begin", "rs1", 3), ("mean", 3, 0), ("mid", "rs1", 2),
    ("fin", "ag1", 0), ("up", 0, 0), ("mid", "ag1", 1), ("up", 0, 1), ("dn", 0, 0), ("dn", 0, 1), ("mid", "rs1", 3),
    ("begin", "rs2", 0), ("fin", "rs1", 2), ("begin", "ag1", 2), ("fin", "ag1", 1), ("up", 1, 0), ("fin", "rs1", 3),
    ("begin", "ag1", 3), ("up", 1, 1), ("mid", "rs2", 0), ("dn", 1, 0), ("dn", 1, 1), ("mid", "ag1", 2),
    ("begin", "rs2", 1), ("mid", "ag1", 3), ("fin", "rs2", 0), ("begin", "ag2", 0), ("fin", "ag1", 2), ("up", 2, 0),
    ("mid", "rs2", 1), ("up", 2, 1), ("dn", 2, 0), ("dn", 2, 1), ("fin", "ag1", 3), ("begin", "rs2", 2),
    ("up", 3, 0), ("mid", "ag2", 0), ("up", 3, 1), ("score", 0, 0), ("dn", 3, 0), ("fin", "rs2", 1),
    ("begin", "ag2", 1), ("dn", 3, 1), ("score", 1, 0), ("mid", "rs2", 2), ("begin", "rs2", 3), ("score", 2, 0),
    ("fin", "ag2", 0), ("mid", "ag2", 1), ("fin", "rs2", 2), ("score", 3, 0), ("begin", "ag2", 2), ("mid", "rs2", 3),
    ("fin", "ag2", 1), ("score", 4, 0), ("mid", "ag2", 2), ("fin", "rs2", 3), ("score", 5, 0), ("begin", "ag2", 3),
    ("fin", "ag2", 2), ("mid", "ag2", 3), ("fin", "ag2", 3),
)
UNITS = tuple((op[1], op[2]) for op in PROGRAM if op[0] == "begin")
N_TILES = {"qkv": 4, "o": 2, "up": 4, "dn": 4}


def rope_lanes(positions):
    half_rot = ROT_DIM // 2
    lane = np.arange(HEAD_DIM)
    inv_freq = np.where(lane < ROT_DIM, ROPE_BASE ** (-2.0 * (lane % half_rot) / ROT_DIM), 0.0).astype(np.float32)
    sign = np.where(lane < half_rot, -1.0, 1.0).astype(np.float32)
    angle = positions.astype(jnp.float32)[:, None] * inv_freq[None, :]
    return jnp.cos(angle), sign[None, :] * jnp.sin(angle)


def layer_kernel(
    n_tp, n_dp, cos_ref, sin_ref, gain1_ref, bias1_ref, gain2_ref, bias2_ref,
    hid_ref, wq_ref, wk_ref, wv_ref, wo_ref, wup_ref, wdn_ref,
    y_ref, score_ref,
    wbuf, part, rbuf, gath, hin, qkv, attn, hmid, act, xmid, ystage, norm_ref, nsq, esq, hsq, sbuf, xbuf,
    wsem, vsem, ssem, rsem, hsem, xsem, ysem, xssem, xrsem,
):
    me = lax.axis_index("tp")
    my_dp = lax.axis_index("dp")
    right = lax.rem(me + 1, n_tp)
    left = lax.rem(me + n_tp - 1, n_tp)
    opp = lax.rem(me + 2, n_tp)
    n_seq = part.shape[1]
    width = part.shape[2]
    blk = n_seq // n_tp
    half = blk // 2
    k_o = wo_ref.shape[0]
    partners = []
    step = 1
    while step < n_dp:
        bit = lax.rem(my_dp // step, 2)
        partners.append(my_dp + step - 2 * step * bit)
        step *= 2

    def half_rows(owner, which):
        return pl.ds(pl.multiple_of(owner * blk + which * half, half), half)

    pieces = [op for op in PROGRAM if op[0] in N_TILES]
    n_q = wq_ref.shape[1]
    n_kv = wk_ref.shape[1]
    n_qkv = n_q + 2 * n_kv
    q_tiles = n_q // TILE
    group = n_q // n_kv
    bases = {}
    base = 0
    for piece in pieces:
        bases[piece] = base
        base += N_TILES[piece[0]]

    def tile_slot(piece, i):
        return lax.rem(bases[piece] + i, NSLOT)

    def columns(i):
        return pl.ds(pl.multiple_of(i * TILE, TILE), TILE)

    def tile_copies(piece, i):
        kind, _, part_no = piece
        slot = tile_slot(piece, i)
        if kind == "o":
            first = 2 * (N_TILES[kind] * part_no + i)
            return (
                pltpu.make_async_copy(wo_ref.at[:, columns(first)], wbuf.at[slot, pl.ds(0, k_o), :], wsem.at[slot]),
                pltpu.make_async_copy(
                    wo_ref.at[:, columns(first + 1)], wbuf.at[slot, pl.ds(k_o, k_o), :], vsem.at[slot]
                ),
            )
        src = {"qkv": wq_ref, "up": wup_ref, "dn": wdn_ref}[kind]
        tile = N_TILES[kind] * part_no + i
        return (pltpu.make_async_copy(src.at[:, columns(tile)], wbuf.at[slot], wsem.at[slot]),)

    def kv_copies(piece):
        slot = tile_slot(piece, q_tiles)
        return (
            pltpu.make_async_copy(wk_ref, wbuf.at[slot, :, pl.ds(0, n_kv)], wsem.at[slot]),
            pltpu.make_async_copy(wv_ref, wbuf.at[slot, :, pl.ds(n_kv, n_kv)], vsem.at[slot]),
        )

    def start_all(copies_of_tile):
        for copy in copies_of_tile:
            copy.start()

    def look_ahead(piece, i):
        tiles = N_TILES[piece[0]]
        after = pieces.index(piece) + 1
        following = pieces[after] if after < len(pieces) else None
        static = isinstance(i, int)

        def when(cond, do):
            if static:
                if cond:
                    do()
            else:
                pl.when(cond)(do)

        if piece[0] == "qkv":
            when(i + 2 < q_tiles, lambda: start_all(tile_copies(piece, i + 2)))
            when(i + 2 == q_tiles, lambda: start_all(kv_copies(piece)))
        else:
            when(i + 2 < tiles, lambda: start_all(tile_copies(piece, i + 2)))
        if following is not None:
            for j in range(2):
                when(i == tiles - 2 + j, lambda j=j: start_all(tile_copies(following, j)))

    def norm_rows(rows, which):
        mean = jnp.sum(rows, axis=-1, keepdims=True) * (1.0 / width)
        centered = rows - mean
        var = jnp.sum(centered * centered, axis=-1, keepdims=True) * (1.0 / width)
        scaled = centered * lax.rsqrt(var + LN_EPS)
        out = scaled * norm_ref[pl.ds(2 * which, 1), :] + norm_ref[pl.ds(2 * which + 1, 1), :]
        return out.astype(jnp.bfloat16)

    def seq_copy(seq):
        return pltpu.make_async_copy(hid_ref.at[seq], ystage.at[seq % 2], xsem.at[seq % 2])

    def first_norm(seq):
        seq_copy(seq).wait()

        def rows_body(i, carry):
            rows = pl.ds(pl.multiple_of(i * 16, 16), 16)
            hin[rows, :] = norm_rows(ystage[seq % 2, rows, :].astype(jnp.float32), 0)
            return carry

        lax.fori_loop(0, n_seq // 16, rows_body, 0)
        if seq + 2 < hid_ref.shape[0]:
            seq_copy(seq + 2).start()

    def first_means():
        def cols_body(i, carry):
            cols = pl.ds(pl.multiple_of(i * TILE, TILE), TILE)
            mean = jnp.sum(hin[:, cols].astype(jnp.float32), axis=0, keepdims=True) * (1.0 / n_seq)
            esq[:, cols] += mean * mean
            return carry

        lax.fori_loop(0, width // TILE, cols_body, 0)

    def rotate(raw, lane):
        rot_half = ROT_DIM // 2
        val = raw.astype(jnp.float32)
        ahead = pltpu.roll(val, HEAD_DIM - rot_half, 1)
        behind = pltpu.roll(val, rot_half, 1)
        partner = jnp.where(lane < rot_half, ahead, behind)
        return (val * cos_ref[...] + partner * sin_ref[...]).astype(jnp.bfloat16)

    def attend():
        lane = lax.broadcasted_iota(jnp.int32, (n_seq, HEAD_DIM), 1)
        row = lax.broadcasted_iota(jnp.int32, (n_seq, n_seq), 0)
        col = lax.broadcasted_iota(jnp.int32, (n_seq, n_seq), 1)
        lane_row = lax.broadcasted_iota(jnp.int32, (1, HEAD_DIM), 1)

        def group_body(g, carry):
            def head_cols(start):
                return pl.ds(pl.multiple_of(start, HEAD_DIM), HEAD_DIM)

            keys = rotate(qkv[:, head_cols(n_q + g * HEAD_DIM)], lane)
            vals = qkv[:, head_cols(n_q + n_kv + g * HEAD_DIM)]
            queries = jnp.concatenate(
                [rotate(qkv[:, head_cols((g * group + i) * HEAD_DIM)], lane) for i in range(group)], axis=0
            )
            scores = lax.dot_general(
                queries, keys, (((1,), (1,)), ((), ())), preferred_element_type=jnp.float32
            ) * HEAD_DIM ** -0.5
            probs = []
            for i in range(group):
                masked = jnp.where(row >= col, scores[i * n_seq : (i + 1) * n_seq], -1e30)
                exps = jnp.exp(masked - jnp.max(masked, axis=-1, keepdims=True))
                probs.append((exps * (1.0 / jnp.sum(exps, axis=-1, keepdims=True))).astype(jnp.bfloat16))
            outs = jnp.dot(
                jnp.concatenate(probs, axis=0), vals, preferred_element_type=jnp.float32
            ).astype(jnp.bfloat16)
            head_sum = jnp.zeros((1, HEAD_DIM), jnp.float32)
            for i in range(group):
                out = outs[i * n_seq : (i + 1) * n_seq]
                attn[:, head_cols((g * group + i) * HEAD_DIM)] = out
                out32 = out.astype(jnp.float32)
                norm = jnp.sqrt(jnp.sum(out32 * out32, axis=-1, keepdims=True))
                mean = jnp.sum(norm, axis=0, keepdims=True) * (1.0 / n_seq)
                head_sum += jnp.where(lane_row == g * group + i, mean * mean, 0.0)
            hsq[...] += head_sum
            return carry

        lax.fori_loop(0, n_kv // HEAD_DIM, group_body, 0)

    def run_piece(piece):
        kind, seq, part_no = piece
        if kind == "qkv":
            first_norm(seq)

        def body(i, carry):
            for copy in tile_copies(piece, i):
                copy.wait()
            look_ahead(piece, i)
            slot = tile_slot(piece, i)
            tile = N_TILES[kind] * part_no + i
            if kind == "qkv":
                qkv[:, columns(i)] = jnp.dot(
                    hin[...], wbuf[slot], preferred_element_type=jnp.float32
                ).astype(jnp.bfloat16)
            elif kind == "o":
                for j in range(2):
                    part[seq % 3, :, columns(2 * tile + j)] = jnp.dot(
                        attn[...], wbuf[slot, pl.ds(j * k_o, k_o), :], preferred_element_type=jnp.float32
                    )
            elif kind == "up":
                up = jnp.maximum(jnp.dot(hmid[...], wbuf[slot], preferred_element_type=jnp.float32), 0.0)
                sq = up * up
                mean = jnp.sum(sq, axis=0, keepdims=True) * (1.0 / n_seq)
                nsq[:, columns(tile)] += mean * mean
                act[:, columns(tile)] = sq.astype(jnp.bfloat16)
            else:
                part[(4 + seq) % 3, :, columns(tile)] = jnp.dot(
                    act[...], wbuf[slot], preferred_element_type=jnp.float32
                )
            return carry

        lax.fori_loop(0, q_tiles if kind == "qkv" else N_TILES[kind], body, 0)
        if kind == "qkv":
            for copy in kv_copies(piece):
                copy.wait()
            look_ahead(piece, q_tiles)
            qkv[:, pl.ds(n_q, 2 * n_kv)] = jnp.dot(
                hin[...], wbuf[tile_slot(piece, q_tiles)], preferred_element_type=jnp.float32
            ).astype(jnp.bfloat16)

    def remote(src, dst, k, direction, j):
        return pltpu.make_async_remote_copy(
            src_ref=src, dst_ref=dst, send_sem=ssem.at[k, direction, j], recv_sem=rsem.at[k, direction, j],
            device_id={"tp": right if direction == 0 else left}, device_id_type=MESH,
        )

    def unit_copies(k):
        kind, seq = UNITS[k]
        ix = seq if kind[2] == "1" else 4 + seq
        if kind[:2] == "rs":
            p = ix % 3
            routes = (
                ((opp, 0), (right, 1), (right, 0)),
                ((opp, 1), (left, 0), (left, 1)),
            )
            return [
                [
                    remote(part.at[p, half_rows(*routes[d][j]), :], rbuf.at[ix, d, j], k, d, j)
                    for j in range(3)
                ]
                for d in range(2)
            ]
        routes = (
            ((me, 0), (me, 1), (left, 0)),
            ((me, 1), (me, 0), (right, 1)),
        )
        return [
            [
                remote(
                    gath.at[ix, half_rows(*routes[d][j]), :], gath.at[ix, half_rows(*routes[d][j]), :], k, d, j
                )
                for j in range(3)
            ]
            for d in range(2)
        ]

    copies = [unit_copies(k) for k in range(len(UNITS))]

    def begin(k):
        for j in range(2):
            for d in range(2):
                copies[k][d][j].start()

    def middle(k):
        kind, seq = UNITS[k]
        ix = seq if kind[2] == "1" else 4 + seq
        for d in range(2):
            copies[k][d][0].wait_recv()
            if kind[:2] == "rs":
                rows = half_rows(right if d == 0 else left, d)
                part[ix % 3, rows, :] = part[ix % 3, rows, :] + rbuf[ix, d, 0]
            copies[k][d][2].start()

    def finish(k):
        kind, seq = UNITS[k]
        ix = seq if kind[2] == "1" else 4 + seq
        for d in range(2):
            for j in (1, 2):
                copies[k][d][j].wait_recv()
        if kind[:2] == "rs":
            for w in range(2):
                rows = half_rows(me, w)
                total = part[ix % 3, rows, :] + rbuf[ix, w, 2] + rbuf[ix, 1 - w, 1]
                mine = pl.ds(w * half, half)
                mid = (xmid[seq, mine, :].astype(jnp.float32) + total).astype(jnp.bfloat16)
                if kind == "rs1":
                    xmid[seq, mine, :] = mid
                    gath[ix, rows, :] = norm_rows(mid.astype(jnp.float32), 1).astype(jnp.float32)
                else:
                    gath[ix, rows, :] = mid.astype(jnp.float32)
        elif kind == "ag1":
            def cast(i, carry):
                cols = pl.ds(pl.multiple_of(i * TILE, TILE), TILE)
                got = gath[ix, :, cols]
                mean = jnp.sum(got, axis=0, keepdims=True) * (1.0 / n_seq)
                esq[:, cols] += mean * mean
                hmid[:, cols] = got.astype(jnp.bfloat16)
                return carry

            lax.fori_loop(0, width // TILE, cast, 0)
        else:
            if seq >= 2:
                y_copy(seq - 2).wait()

            def store(i, carry):
                cols = pl.ds(pl.multiple_of(i * TILE, TILE), TILE)
                ystage[seq % 2, :, cols] = gath[ix, :, cols].astype(jnp.bfloat16)
                return carry

            lax.fori_loop(0, width // TILE, store, 0)
            y_copy(seq).start()
        for d in range(2):
            for j in range(3):
                copies[k][d][j].wait_send()

    def y_copy(seq):
        return pltpu.make_async_copy(ystage.at[seq % 2], y_ref.at[seq], ysem.at[seq % 2])

    def score_copy(i):
        return pltpu.make_async_remote_copy(
            src_ref=sbuf.at[i], dst_ref=xbuf.at[i], send_sem=xssem.at[i], recv_sem=xrsem.at[i],
            device_id={"dp": partners[i]}, device_id_type=MESH,
        )

    def score_begin():
        n_rows, e_rows = nsq.shape[1] // 128, width // 128
        for r in range(n_rows):
            sbuf[0, r : r + 1, :] = nsq[:, r * 128 : (r + 1) * 128]
        for r in range(e_rows):
            sbuf[0, n_rows + r : n_rows + r + 1, :] = esq[:, r * 128 : (r + 1) * 128]
        sbuf[0, n_rows + e_rows :, :] = jnp.broadcast_to(hsq[...], (8, 128))
        score_copy(0).start()

    def score_step(i):
        score_copy(i).wait()
        sbuf[i + 1] = sbuf[i] + xbuf[i]
        if i + 1 < len(partners):
            score_copy(i + 1).start()

    def read_norm(which, gain_ref, bias_ref):
        gain = 1.0 + gain_ref[...].astype(jnp.float32)
        bias = bias_ref[...].astype(jnp.float32)
        for r in range(width // 128):
            cols = slice(r * 128, (r + 1) * 128)
            norm_ref[2 * which : 2 * which + 1, cols] = gain[r : r + 1, :]
            norm_ref[2 * which + 1 : 2 * which + 2, cols] = bias[r : r + 1, :]

    seq_copy(0).start()
    for i in range(2):
        start_all(tile_copies(pieces[0], i))
    seq_copy(1).start()
    hid_copies = [
        pltpu.make_async_copy(
            hid_ref.at[seq, pl.ds(pl.multiple_of(me * blk, blk), blk), :], xmid.at[seq], hsem.at[seq]
        )
        for seq in range(hid_ref.shape[0])
    ]
    for copy in hid_copies:
        copy.start()

    barrier = pltpu.get_barrier_semaphore()
    for t in (left, right):
        pl.semaphore_signal(barrier, inc=1, device_id={"tp": t}, device_id_type=MESH)
    for other in partners:
        pl.semaphore_signal(barrier, inc=1, device_id={"dp": other}, device_id_type=MESH)
    read_norm(0, gain1_ref, bias1_ref)
    nsq[...] = jnp.zeros_like(nsq)
    esq[...] = jnp.zeros_like(esq)
    hsq[...] = jnp.zeros_like(hsq)

    for op in PROGRAM:
        name, arg, no = op
        if name in N_TILES:
            run_piece(op)
        elif name == "att":
            attend()
        elif name == "mean":
            first_means()
        elif name == "begin":
            k = UNITS.index((arg, no))
            if k == 0:
                pl.semaphore_wait(barrier, 2 + len(partners))
            begin(k)
            if k == 0:
                read_norm(1, gain2_ref, bias2_ref)
                for copy in hid_copies:
                    copy.wait()
        elif name == "mid":
            middle(UNITS.index((arg, no)))
        elif name == "fin":
            finish(UNITS.index((arg, no)))
        elif arg == 0:
            score_begin()
        else:
            score_step(arg - 1)
    score_ref[...] = jnp.sqrt(sbuf[len(partners)])
    for seq in (2, 3):
        y_copy(seq).wait()


def final_kernel(n_rows, e_rows, y_ref, score_ref, out_ref, neuron_ref, embed_ref, head_ref, stage, in_sem, out_sem):
    n_batch = y_ref.shape[0]
    loads = [pltpu.make_async_copy(y_ref.at[i], stage.at[i], in_sem.at[i]) for i in range(n_batch)]
    stores = [pltpu.make_async_copy(stage.at[i], out_ref.at[i], out_sem.at[i]) for i in range(n_batch)]
    for load in loads:
        load.start()
    neuron_ref[...] = score_ref[:n_rows, :]
    embed_ref[...] = score_ref[n_rows : n_rows + e_rows, :]
    head_ref[...] = score_ref[n_rows + e_rows : n_rows + e_rows + 1, : head_ref.shape[1]]
    for load, store in zip(loads, stores):
        load.wait()
        store.start()
    for store in stores:
        store.wait()


def solution(mesh):
    n_tp = mesh.shape["tp"]
    n_dp = mesh.shape["dp"]

    def local_layer(hidden, positions, ln1_gain, ln1_bias, w_q, w_k, w_v, w_o, ln2_gain, ln2_bias, w_up, w_down):
        n_batch, n_seq, width = hidden.shape
        ff_local = w_up.shape[1]
        heads_local = w_q.shape[1] // HEAD_DIM
        cos_l, sin_l = rope_lanes(positions)
        norm_params = [p.reshape(width // 128, 128) for p in (ln1_gain, ln1_bias, ln2_gain, ln2_bias)]
        n_rows, e_rows = ff_local // 128, width // 128
        score_rows = n_rows + e_rows + 8
        n_stage = n_dp.bit_length() - 1
        blk = n_seq // n_tp
        any_spec = pl.BlockSpec(memory_space=pl.ANY)
        vmem_spec = pl.BlockSpec(memory_space=pltpu.VMEM)
        n_units = len(UNITS)
        y, score = pl.pallas_call(
            functools.partial(layer_kernel, n_tp, n_dp),
            out_shape=(
                jax.ShapeDtypeStruct(hidden.shape, jnp.bfloat16),
                jax.ShapeDtypeStruct((score_rows, 128), jnp.float32),
            ),
            in_specs=[vmem_spec] * 6 + [any_spec] * 7,
            out_specs=(any_spec, vmem_spec),
            scratch_shapes=[
                pltpu.VMEM((NSLOT, width, TILE), jnp.bfloat16),
                pltpu.VMEM((3, n_seq, width), jnp.float32),
                pltpu.VMEM((2 * n_batch, 2, 3, blk // 2, width), jnp.float32),
                pltpu.VMEM((2 * n_batch, n_seq, width), jnp.float32),
                pltpu.VMEM((n_seq, width), jnp.bfloat16),
                pltpu.VMEM((n_seq, w_q.shape[1] + 2 * w_k.shape[1]), jnp.bfloat16),
                pltpu.VMEM((n_seq, w_q.shape[1]), jnp.bfloat16),
                pltpu.VMEM((n_seq, width), jnp.bfloat16),
                pltpu.VMEM((n_seq, ff_local), jnp.bfloat16),
                pltpu.VMEM((n_batch, blk, width), jnp.bfloat16),
                pltpu.VMEM((2, n_seq, width), jnp.bfloat16),
                pltpu.VMEM((4, width), jnp.float32),
                pltpu.VMEM((1, ff_local), jnp.float32),
                pltpu.VMEM((1, width), jnp.float32),
                pltpu.VMEM((1, 128), jnp.float32),
                pltpu.VMEM((n_stage + 1, score_rows, 128), jnp.float32),
                pltpu.VMEM((n_stage, score_rows, 128), jnp.float32),
                pltpu.SemaphoreType.DMA((NSLOT,)),
                pltpu.SemaphoreType.DMA((NSLOT,)),
                pltpu.SemaphoreType.DMA((n_units, 2, 3)),
                pltpu.SemaphoreType.DMA((n_units, 2, 3)),
                pltpu.SemaphoreType.DMA((n_batch,)),
                pltpu.SemaphoreType.DMA((2,)),
                pltpu.SemaphoreType.DMA((2,)),
                pltpu.SemaphoreType.DMA((n_stage,)),
                pltpu.SemaphoreType.DMA((n_stage,)),
            ],
            compiler_params=pltpu.CompilerParams(
                collective_id=0, has_side_effects=True, vmem_limit_bytes=66_000_000
            ),
            name="layer",
        )(cos_l, sin_l, *norm_params, hidden, w_q, w_k, w_v, w_o, w_up, w_down)
        y, neuron, embed, head = pl.pallas_call(
            functools.partial(final_kernel, n_rows, e_rows),
            out_shape=(
                jax.ShapeDtypeStruct(hidden.shape, jnp.bfloat16),
                jax.ShapeDtypeStruct((n_rows, 128), jnp.float32),
                jax.ShapeDtypeStruct((e_rows, 128), jnp.float32),
                jax.ShapeDtypeStruct((1, heads_local), jnp.float32),
            ),
            in_specs=[any_spec, vmem_spec],
            out_specs=(any_spec, vmem_spec, vmem_spec, vmem_spec),
            scratch_shapes=[
                pltpu.VMEM(hidden.shape, jnp.bfloat16),
                pltpu.SemaphoreType.DMA((n_batch,)),
                pltpu.SemaphoreType.DMA((n_batch,)),
            ],
            name="final",
        )(y, score)
        return y, neuron.reshape(ff_local), head.reshape(heads_local), embed.reshape(width)

    weight_col = P(None, "tp")
    weight_row = P("tp", None)
    return jax.shard_map(
        local_layer,
        mesh=mesh,
        in_specs=(P("dp"), P(), P(), P(), weight_col, weight_col, weight_col, weight_row, P(), P(), weight_col, weight_row),
        out_specs=(P("dp"), P("tp"), P("tp"), P()),
        check_vma=False,
    )
```

```python
import functools

import jax
import jax.numpy as jnp
import numpy as np
from jax import lax
from jax.experimental import pallas as pl
from jax.experimental.pallas import tpu as pltpu
from jax.sharding import PartitionSpec as P

HEAD_DIM = 128
ROT_DIM = 64
ROPE_BASE = 10000.0
LN_EPS = 1e-5
TILE = 512
NSLOT = 3
VMEM_LIMIT = 66_000_000
MESH = pl.DeviceIdType.MESH

PROGRAM = (
    ("qkv", 0, 0), ("att", 0, 0), ("o", 0, 0), ("early", "rs1", 0), ("o", 0, 1), ("begin", "rs1", 0), ("mean", 0, 0),
    ("qkv", 1, 0), ("att", 1, 0), ("mid", "rs1", 0), ("o", 1, 0), ("o", 1, 1), ("begin", "rs1", 1), ("mean", 1, 0),
    ("qkv", 2, 0), ("att", 2, 0), ("fin", "rs1", 0), ("begin", "ag1", 0), ("o", 2, 0), ("o", 2, 1),
    ("mid", "rs1", 1), ("mean", 2, 0), ("qkv", 3, 0), ("begin", "rs1", 2), ("att", 3, 0), ("o", 3, 0), ("o", 3, 1),
    ("mid", "ag1", 0), ("mean", 3, 0), ("begin", "rs1", 3), ("fin", "rs1", 1), ("mid", "rs1", 2),
    ("begin", "ag1", 1), ("fin", "ag1", 0), ("up", 0, 0), ("mid", "rs1", 3), ("up", 0, 1), ("dn", 0, 0),
    ("dn", 0, 1), ("fin", "rs1", 2), ("mid", "ag1", 1), ("begin", "ag1", 2), ("begin", "rs2", 0), ("fin", "rs1", 3),
    ("fin", "ag1", 1), ("up", 1, 0), ("mid", "ag1", 2), ("up", 1, 1), ("begin", "ag1", 3), ("dn", 1, 0),
    ("dn", 1, 1), ("mid", "rs2", 0), ("begin", "rs2", 1), ("fin", "ag1", 2), ("up", 2, 0), ("mid", "ag1", 3),
    ("up", 2, 1), ("dn", 2, 0), ("dn", 2, 1), ("fin", "rs2", 0), ("mid", "rs2", 1), ("begin", "ag2", 0),
    ("begin", "rs2", 2), ("fin", "ag1", 3), ("up", 3, 0), ("fin", "rs2", 1), ("up", 3, 1), ("score", 0, 0),
    ("mid", "ag2", 0), ("dn", 3, 0), ("begin", "ag2", 1), ("score", 1, 0), ("dn", 3, 1), ("mid", "rs2", 2),
    ("begin", "rs2", 3), ("score", 2, 0), ("fin", "ag2", 0), ("mid", "ag2", 1), ("fin", "rs2", 2), ("score", 3, 0),
    ("begin", "ag2", 2), ("mid", "rs2", 3), ("fin", "ag2", 1), ("score", 4, 0), ("mid", "ag2", 2), ("fin", "rs2", 3),
    ("begin", "ag2", 3), ("score", 5, 0), ("fin", "ag2", 2), ("mid", "ag2", 3), ("fin", "ag2", 3),
)
UNITS = tuple((op[1], op[2]) for op in PROGRAM if op[0] == "begin")
N_TILES = {"qkv": 4, "o": 2, "up": 4, "dn": 4}


def rope_rows():
    half_rot = ROT_DIM // 2
    lane = np.arange(HEAD_DIM)
    inv_freq = np.where(lane < ROT_DIM, ROPE_BASE ** (-2.0 * (lane % half_rot) / ROT_DIM), 0.0)
    return np.stack([inv_freq, np.where(lane < half_rot, -1.0, 1.0)]).astype(np.float32)


def layer_kernel(
    n_tp, n_dp, pos_in, freq_in, gain1_in, bias1_in, gain2_in, bias2_in,
    hid_ref, wq_ref, wk_ref, wv_ref, wo_ref, wup_ref, wdn_ref,
    y_ref, score_ref,
    wbuf, part, rbuf, gath, hin, qkv, attn, hmid, act, xmid, ystage, pos_ref, freq_ref, rope_ref, raw_ref, norm_ref, nsq, esq, hsq, sbuf, xbuf,
    wsem, vsem, ssem, rsem, esend, erecv, psem, bsem, osem, hsem, xsem, ysem, xssem, xrsem,
):
    me = lax.axis_index("tp")
    my_dp = lax.axis_index("dp")
    right = lax.rem(me + 1, n_tp)
    left = lax.rem(me + n_tp - 1, n_tp)
    opp = lax.rem(me + 2, n_tp)
    n_seq = part.shape[1]
    width = part.shape[2]
    blk = n_seq // n_tp
    half = blk // 2
    k_o = wo_ref.shape[0]
    partners = []
    step = 1
    while step < n_dp:
        bit = lax.rem(my_dp // step, 2)
        partners.append(my_dp + step - 2 * step * bit)
        step *= 2

    def half_rows(owner, which):
        return pl.ds(pl.multiple_of(owner * blk + which * half, half), half)

    pieces = [op for op in PROGRAM if op[0] in N_TILES]
    n_q = wq_ref.shape[1]
    n_kv = wk_ref.shape[1]
    n_qkv = n_q + 2 * n_kv
    q_tiles = n_q // TILE
    group = n_q // n_kv
    bases = {}
    base = 0
    for piece in pieces:
        bases[piece] = base
        base += N_TILES[piece[0]]

    def tile_slot(piece, i):
        return lax.rem(bases[piece] + i, NSLOT)

    def columns(i):
        return pl.ds(pl.multiple_of(i * TILE, TILE), TILE)

    def tile_copies(piece, i):
        kind, _, part_no = piece
        slot = tile_slot(piece, i)
        if kind == "o":
            first = 2 * (N_TILES[kind] * part_no + i)
            return (
                pltpu.make_async_copy(wo_ref.at[:, columns(first)], wbuf.at[slot, pl.ds(0, k_o), :], wsem.at[slot]),
                pltpu.make_async_copy(
                    wo_ref.at[:, columns(first + 1)], wbuf.at[slot, pl.ds(k_o, k_o), :], vsem.at[slot]
                ),
            )
        src = {"qkv": wq_ref, "up": wup_ref, "dn": wdn_ref}[kind]
        tile = N_TILES[kind] * part_no + i
        return (pltpu.make_async_copy(src.at[:, columns(tile)], wbuf.at[slot], wsem.at[slot]),)

    def kv_copies(piece):
        slot = tile_slot(piece, q_tiles)
        return (
            pltpu.make_async_copy(wk_ref, wbuf.at[slot, :, pl.ds(0, n_kv)], wsem.at[slot]),
            pltpu.make_async_copy(wv_ref, wbuf.at[slot, :, pl.ds(n_kv, n_kv)], vsem.at[slot]),
        )

    def start_all(copies_of_tile):
        for copy in copies_of_tile:
            copy.start()

    def start_tile(number):
        for piece in pieces:
            tile = number - bases[piece]
            if 0 <= tile < N_TILES[piece[0]]:
                is_kv = piece[0] == "qkv" and tile == q_tiles
                start_all(kv_copies(piece) if is_kv else tile_copies(piece, tile))

    def look_ahead(piece, i):
        if isinstance(i, int):
            start_tile(bases[piece] + i + NSLOT)
            return
        for j in range(q_tiles if piece[0] == "qkv" else N_TILES[piece[0]]):

            @pl.when(i == j)
            def _(j=j):
                start_tile(bases[piece] + j + NSLOT)

    def norm_rows(rows, which):
        mean = jnp.sum(rows, axis=-1, keepdims=True) * (1.0 / width)
        centered = rows - mean
        var = jnp.sum(centered * centered, axis=-1, keepdims=True) * (1.0 / width)
        scaled = centered * lax.rsqrt(var + LN_EPS)
        out = scaled * norm_ref[pl.ds(2 * which, 1), :] + norm_ref[pl.ds(2 * which + 1, 1), :]
        return out.astype(jnp.bfloat16)

    def seq_copy(seq):
        return pltpu.make_async_copy(hid_ref.at[seq], ystage.at[seq % 2], xsem.at[seq % 2])

    def first_norm(seq):
        seq_copy(seq).wait()

        def rows_body(i, carry):
            rows = pl.ds(pl.multiple_of(i * 16, 16), 16)
            hin[rows, :] = norm_rows(ystage[seq % 2, rows, :].astype(jnp.float32), 0)
            return carry

        lax.fori_loop(0, n_seq // 16, rows_body, 0)
        if seq + 2 < hid_ref.shape[0]:
            seq_copy(seq + 2).start()

    def first_means():
        def cols_body(i, carry):
            cols = pl.ds(pl.multiple_of(i * TILE, TILE), TILE)
            mean = jnp.sum(hin[:, cols].astype(jnp.float32), axis=0, keepdims=True) * (1.0 / n_seq)
            esq[:, cols] += mean * mean
            return carry

        lax.fori_loop(0, width // TILE, cols_body, 0)

    def rotate(raw, lane):
        rot_half = ROT_DIM // 2
        val = raw.astype(jnp.float32)
        ahead = pltpu.roll(val, HEAD_DIM - rot_half, 1)
        behind = pltpu.roll(val, rot_half, 1)
        partner = jnp.where(lane < rot_half, ahead, behind)
        return (val * rope_ref[0] + partner * rope_ref[1]).astype(jnp.bfloat16)

    def attend():
        lane = lax.broadcasted_iota(jnp.int32, (n_seq, HEAD_DIM), 1)
        row = lax.broadcasted_iota(jnp.int32, (n_seq, n_seq), 0)
        col = lax.broadcasted_iota(jnp.int32, (n_seq, n_seq), 1)
        lane_row = lax.broadcasted_iota(jnp.int32, (1, HEAD_DIM), 1)

        def group_body(g, carry):
            def head_cols(start):
                return pl.ds(pl.multiple_of(start, HEAD_DIM), HEAD_DIM)

            keys = rotate(qkv[:, head_cols(n_q + g * HEAD_DIM)], lane)
            vals = qkv[:, head_cols(n_q + n_kv + g * HEAD_DIM)]
            queries = jnp.concatenate(
                [rotate(qkv[:, head_cols((g * group + i) * HEAD_DIM)], lane) for i in range(group)], axis=0
            )
            scores = lax.dot_general(
                queries, keys, (((1,), (1,)), ((), ())), preferred_element_type=jnp.float32
            ) * HEAD_DIM ** -0.5
            probs = []
            for i in range(group):
                masked = jnp.where(row >= col, scores[i * n_seq : (i + 1) * n_seq], -1e30)
                exps = jnp.exp(masked - jnp.max(masked, axis=-1, keepdims=True))
                probs.append((exps * (1.0 / jnp.sum(exps, axis=-1, keepdims=True))).astype(jnp.bfloat16))
            outs = jnp.dot(
                jnp.concatenate(probs, axis=0), vals, preferred_element_type=jnp.float32
            ).astype(jnp.bfloat16)
            head_sum = jnp.zeros((1, HEAD_DIM), jnp.float32)
            for i in range(group):
                out = outs[i * n_seq : (i + 1) * n_seq]
                attn[:, head_cols((g * group + i) * HEAD_DIM)] = out
                out32 = out.astype(jnp.float32)
                norm = jnp.sqrt(jnp.sum(out32 * out32, axis=-1, keepdims=True))
                mean = jnp.sum(norm, axis=0, keepdims=True) * (1.0 / n_seq)
                head_sum += jnp.where(lane_row == g * group + i, mean * mean, 0.0)
            hsq[...] += head_sum
            return carry

        lax.fori_loop(0, n_kv // HEAD_DIM, group_body, 0)

    def run_piece(piece):
        kind, seq, part_no = piece
        if kind == "qkv":
            first_norm(seq)

        def body(i, carry):
            for copy in tile_copies(piece, i):
                copy.wait()
            slot = tile_slot(piece, i)
            tile = N_TILES[kind] * part_no + i
            if kind == "qkv":
                qkv[:, columns(i)] = jnp.dot(
                    hin[...], wbuf[slot], preferred_element_type=jnp.float32
                ).astype(jnp.bfloat16)
            elif kind == "o":
                for j in range(2):
                    part[seq % 3, :, columns(2 * tile + j)] = jnp.dot(
                        attn[...], wbuf[slot, pl.ds(j * k_o, k_o), :], preferred_element_type=jnp.float32
                    )
            elif kind == "up":
                up = jnp.maximum(jnp.dot(hmid[...], wbuf[slot], preferred_element_type=jnp.float32), 0.0)
                sq = up * up
                mean = jnp.sum(sq, axis=0, keepdims=True) * (1.0 / n_seq)
                nsq[:, columns(tile)] += mean * mean
                act[:, columns(tile)] = sq.astype(jnp.bfloat16)
            else:
                part[(4 + seq) % 3, :, columns(tile)] = jnp.dot(
                    act[...], wbuf[slot], preferred_element_type=jnp.float32
                )
            look_ahead(piece, i)
            return carry

        lax.fori_loop(0, q_tiles if kind == "qkv" else N_TILES[kind], body, 0)
        if kind == "qkv":
            for copy in kv_copies(piece):
                copy.wait()
            qkv[:, pl.ds(n_q, 2 * n_kv)] = jnp.dot(
                hin[...], wbuf[tile_slot(piece, q_tiles)], preferred_element_type=jnp.float32
            ).astype(jnp.bfloat16)
            look_ahead(piece, q_tiles)

    def remote(src, dst, k, direction, j):
        return pltpu.make_async_remote_copy(
            src_ref=src, dst_ref=dst, send_sem=ssem.at[k, direction, j], recv_sem=rsem.at[k, direction, j],
            device_id={"tp": right if direction == 0 else left}, device_id_type=MESH,
        )

    def unit_copies(k):
        kind, seq = UNITS[k]
        ix = seq if kind[2] == "1" else 4 + seq
        if kind[:2] == "rs":
            p = ix % 3
            routes = (
                ((opp, 0), (right, 1), (right, 0)),
                ((opp, 1), (left, 0), (left, 1)),
            )
            return [
                [
                    remote(part.at[p, half_rows(*routes[d][j]), :], rbuf.at[ix, d, j], k, d, j)
                    for j in range(3)
                ]
                for d in range(2)
            ]
        routes = (
            ((me, 0), (me, 1), (left, 0)),
            ((me, 1), (me, 0), (right, 1)),
        )
        return [
            [
                remote(
                    gath.at[ix, half_rows(*routes[d][j]), :], gath.at[ix, half_rows(*routes[d][j]), :], k, d, j
                )
                for j in range(3)
            ]
            for d in range(2)
        ]

    copies = [unit_copies(k) for k in range(len(UNITS))]

    def early_copies():
        owners = (((opp, 0), (right, 1)), ((opp, 1), (left, 0)))

        def one(d, j, side):
            cols = pl.ds(side * (width // 2), width // 2)
            sems = (esend, erecv) if side == 0 else (ssem.at[0], rsem.at[0])
            return pltpu.make_async_remote_copy(
                src_ref=part.at[0, half_rows(*owners[d][j]), cols], dst_ref=rbuf.at[0, d, j, :, cols],
                send_sem=sems[0].at[d, j], recv_sem=sems[1].at[d, j],
                device_id={"tp": right if d == 0 else left}, device_id_type=MESH,
            )

        return [[[one(d, j, side) for j in range(2)] for d in range(2)] for side in range(2)]

    early, late = early_copies()
    for d in range(2):
        copies[0][d][:2] = late[d]

    def early_begin():
        for j in range(2):
            for d in range(2):
                early[d][j].start()

    def begin(k):
        for j in range(2):
            for d in range(2):
                copies[k][d][j].start()

    def middle(k):
        kind, seq = UNITS[k]
        ix = seq if kind[2] == "1" else 4 + seq
        for d in range(2):
            if k == 0:
                early[d][0].wait_recv()
            copies[k][d][0].wait_recv()
            if kind[:2] == "rs":
                rows = half_rows(right if d == 0 else left, d)
                part[ix % 3, rows, :] = part[ix % 3, rows, :] + rbuf[ix, d, 0]
            copies[k][d][2].start()

    def finish(k):
        kind, seq = UNITS[k]
        ix = seq if kind[2] == "1" else 4 + seq
        if k == len(UNITS) - 1:
            last_finish(k, seq, ix)
            return
        for d in range(2):
            if k == 0:
                early[d][1].wait_recv()
            for j in (1, 2):
                copies[k][d][j].wait_recv()
        if kind[:2] == "rs":
            for w in range(2):
                rows = half_rows(me, w)
                total = part[ix % 3, rows, :] + rbuf[ix, w, 2] + rbuf[ix, 1 - w, 1]
                mine = pl.ds(w * half, half)
                mid = (xmid[seq, mine, :].astype(jnp.float32) + total).astype(jnp.bfloat16)
                if kind == "rs1":
                    xmid[seq, mine, :] = mid
                    gath[ix, rows, :] = norm_rows(mid.astype(jnp.float32), 1).astype(jnp.float32)
                else:
                    gath[ix, rows, :] = mid.astype(jnp.float32)
        elif kind == "ag1":
            def cast(i, carry):
                cols = pl.ds(pl.multiple_of(i * TILE, TILE), TILE)
                got = gath[ix, :, cols]
                mean = jnp.sum(got, axis=0, keepdims=True) * (1.0 / n_seq)
                esq[:, cols] += mean * mean
                hmid[:, cols] = got.astype(jnp.bfloat16)
                return carry

            lax.fori_loop(0, width // TILE, cast, 0)
        else:
            if seq >= 2:
                y_copy(seq - 2).wait()

            def store(i, carry):
                cols = pl.ds(pl.multiple_of(i * TILE, TILE), TILE)
                ystage[seq % 2, :, cols] = gath[ix, :, cols].astype(jnp.bfloat16)
                return carry

            lax.fori_loop(0, width // TILE, store, 0)
            y_copy(seq).start()
        for d in range(2):
            for j in range(3):
                copies[k][d][j].wait_send()
                if k == 0 and j < 2:
                    early[d][j].wait_send()

    def block_copy(seq, owner, i):
        rows = pl.ds(pl.multiple_of(owner * blk, blk), blk)
        return pltpu.make_async_copy(ystage.at[seq % 2, rows, :], y_ref.at[seq, rows, :], bsem.at[i])

    def last_finish(k, seq, ix):
        y_copy(seq - 2).wait()
        for i, owner in enumerate((me, left, right, opp)):
            rows = pl.ds(pl.multiple_of(owner * blk, blk), blk)
            if i == 1 or i == 3:
                for d in range(2):
                    copies[k][d][1 if i == 1 else 2].wait_recv()

            def store(c, carry, rows=rows):
                ystage[seq % 2, rows, columns(c)] = gath[ix, rows, columns(c)].astype(jnp.bfloat16)
                return carry

            lax.fori_loop(0, width // TILE, store, 0)
            block_copy(seq, owner, i).start()
        for d in range(2):
            for j in range(3):
                copies[k][d][j].wait_send()
        for i, owner in enumerate((me, left, right, opp)):
            block_copy(seq, owner, i).wait()

    def y_copy(seq):
        return pltpu.make_async_copy(ystage.at[seq % 2], y_ref.at[seq], ysem.at[seq % 2])

    def score_copy(i):
        return pltpu.make_async_remote_copy(
            src_ref=sbuf.at[i], dst_ref=xbuf.at[i], send_sem=xssem.at[i], recv_sem=xrsem.at[i],
            device_id={"dp": partners[i]}, device_id_type=MESH,
        )

    def score_begin():
        n_rows, e_rows = nsq.shape[1] // 128, width // 128
        for r in range(n_rows):
            sbuf[0, r : r + 1, :] = nsq[:, r * 128 : (r + 1) * 128]
        for r in range(e_rows):
            sbuf[0, n_rows + r : n_rows + r + 1, :] = esq[:, r * 128 : (r + 1) * 128]
        sbuf[0, n_rows + e_rows :, :] = jnp.broadcast_to(hsq[...], (8, 128))
        score_copy(0).start()

    def score_step(i):
        score_copy(i).wait()
        sbuf[i + 1] = sbuf[i] + xbuf[i]
        if i + 1 < len(partners):
            score_copy(i + 1).start()

    def read_norm(which):
        for i in (2 * which, 2 * which + 1):
            param_copies[i].wait()
        gain = 1.0 + raw_ref[2 * which].astype(jnp.float32)
        bias = raw_ref[2 * which + 1].astype(jnp.float32)
        for r in range(width // 128):
            cols = slice(r * 128, (r + 1) * 128)
            norm_ref[2 * which : 2 * which + 1, cols] = gain[r : r + 1, :]
            norm_ref[2 * which + 1 : 2 * which + 2, cols] = bias[r : r + 1, :]

    def read_rope():
        for copy in param_copies[4:]:
            copy.wait()
        row = lax.broadcasted_iota(jnp.int32, (n_seq, n_seq), 0)
        col = lax.broadcasted_iota(jnp.int32, (n_seq, n_seq), 1)
        pos = jnp.where(row == col, pos_ref[...].astype(jnp.float32), 0.0)
        angle = jnp.sum(pos, axis=1, keepdims=True) * freq_ref[0:1, :]
        rope_ref[0] = jnp.cos(angle)
        rope_ref[1] = freq_ref[1:2, :] * jnp.sin(angle)

    param_copies = [
        pltpu.make_async_copy(src, raw_ref.at[i], psem.at[i])
        for i, src in enumerate((gain1_in, bias1_in, gain2_in, bias2_in))
    ] + [
        pltpu.make_async_copy(pos_in, pos_ref, psem.at[4]),
        pltpu.make_async_copy(freq_in, freq_ref, psem.at[5]),
    ]
    hid_copies = [
        pltpu.make_async_copy(
            hid_ref.at[seq, pl.ds(pl.multiple_of(me * blk, blk), blk), :], xmid.at[seq], hsem.at[seq]
        )
        for seq in range(hid_ref.shape[0])
    ]
    seq_copy(0).start()
    start_all(param_copies)
    start_tile(0)
    for i in range(1, NSLOT):
        start_tile(i)

    barrier = pltpu.get_barrier_semaphore()
    for t in (left, right):
        pl.semaphore_signal(barrier, inc=1, device_id={"tp": t}, device_id_type=MESH)
    for other in partners:
        pl.semaphore_signal(barrier, inc=1, device_id={"dp": other}, device_id_type=MESH)
    read_norm(0)
    read_rope()
    nsq[...] = jnp.zeros_like(nsq)
    esq[...] = jnp.zeros_like(esq)
    hsq[...] = jnp.zeros_like(hsq)

    score_out = pltpu.make_async_copy(sbuf.at[0], score_ref, osem)
    for op in PROGRAM:
        name, arg, no = op
        if name in N_TILES:
            run_piece(op)
        elif name == "att":
            if arg == 0:
                seq_copy(1).start()
            attend()
        elif name == "early":
            pl.semaphore_wait(barrier, 2 + len(partners))
            early_begin()
        elif name == "mean":
            first_means()
        elif name == "begin":
            k = UNITS.index((arg, no))
            begin(k)
            if k == 0:
                start_all(hid_copies)
                read_norm(1)
        elif name == "mid":
            middle(UNITS.index((arg, no)))
        elif name == "fin":
            if (arg, no) == UNITS[0]:
                for copy in hid_copies:
                    copy.wait()
            finish(UNITS.index((arg, no)))
        elif arg == 0:
            score_begin()
        else:
            score_step(arg - 1)
            if arg == len(partners):
                sbuf[0] = jnp.sqrt(sbuf[len(partners)])
                score_out.start()
    y_copy(2).wait()
    score_out.wait()


def final_kernel(
    n_rows, e_rows, y_ref, score_ref, out_ref, neuron_ref, embed_ref, head_ref, stage, scores, heads, in_sem, out_sem
):
    count = y_ref.shape[0]
    loads = [pltpu.make_async_copy(y_ref.at[i], stage.at[i], in_sem.at[i]) for i in range(count)]
    stores = [pltpu.make_async_copy(stage.at[i], out_ref.at[i], out_sem.at[i]) for i in range(count)]
    loads.insert(0, pltpu.make_async_copy(score_ref, scores, in_sem.at[count]))
    score_stores = [
        pltpu.make_async_copy(scores.at[pl.ds(0, n_rows), :], neuron_ref, out_sem.at[count]),
        pltpu.make_async_copy(scores.at[pl.ds(n_rows, e_rows), :], embed_ref, out_sem.at[count + 1]),
        pltpu.make_async_copy(heads, head_ref, out_sem.at[count + 2]),
    ]
    for load in loads:
        load.start()
    loads[0].wait()
    heads[...] = scores[n_rows + e_rows : n_rows + e_rows + 1, : heads.shape[1]]
    for store in score_stores:
        store.start()
    for load, store in zip(loads[1:], stores):
        load.wait()
        store.start()
    for store in score_stores + stores:
        store.wait()


def solution(mesh):
    n_tp = mesh.shape["tp"]
    n_dp = mesh.shape["dp"]

    def local_layer(hidden, positions, ln1_gain, ln1_bias, w_q, w_k, w_v, w_o, ln2_gain, ln2_bias, w_up, w_down):
        n_batch, n_seq, width = hidden.shape
        ff_local = w_up.shape[1]
        heads_local = w_q.shape[1] // HEAD_DIM
        norm_params = [p.reshape(width // 128, 128) for p in (ln1_gain, ln1_bias, ln2_gain, ln2_bias)]
        n_rows, e_rows = ff_local // 128, width // 128
        score_rows = n_rows + e_rows + 8
        n_stage = n_dp.bit_length() - 1
        blk = n_seq // n_tp
        any_spec = pl.BlockSpec(memory_space=pl.ANY)
        n_units = len(UNITS)
        y, score = pl.pallas_call(
            functools.partial(layer_kernel, n_tp, n_dp),
            out_shape=(
                jax.ShapeDtypeStruct(hidden.shape, jnp.bfloat16),
                jax.ShapeDtypeStruct((score_rows, 128), jnp.float32),
            ),
            in_specs=[any_spec] * 13,
            out_specs=(any_spec, any_spec),
            scratch_shapes=[
                pltpu.VMEM((NSLOT, width, TILE), jnp.bfloat16),
                pltpu.VMEM((3, n_seq, width), jnp.float32),
                pltpu.VMEM((2 * n_batch, 2, 3, blk // 2, width), jnp.float32),
                pltpu.VMEM((2 * n_batch, n_seq, width), jnp.float32),
                pltpu.VMEM((n_seq, width), jnp.bfloat16),
                pltpu.VMEM((n_seq, w_q.shape[1] + 2 * w_k.shape[1]), jnp.bfloat16),
                pltpu.VMEM((n_seq, w_q.shape[1]), jnp.bfloat16),
                pltpu.VMEM((n_seq, width), jnp.bfloat16),
                pltpu.VMEM((n_seq, ff_local), jnp.bfloat16),
                pltpu.VMEM((n_batch, blk, width), jnp.bfloat16),
                pltpu.VMEM((2, n_seq, width), jnp.bfloat16),
                pltpu.VMEM((1, n_seq), jnp.int32),
                pltpu.VMEM((2, HEAD_DIM), jnp.float32),
                pltpu.VMEM((2, n_seq, HEAD_DIM), jnp.float32),
                pltpu.VMEM((4, width // 128, 128), jnp.bfloat16),
                pltpu.VMEM((4, width), jnp.float32),
                pltpu.VMEM((1, ff_local), jnp.float32),
                pltpu.VMEM((1, width), jnp.float32),
                pltpu.VMEM((1, 128), jnp.float32),
                pltpu.VMEM((n_stage + 1, score_rows, 128), jnp.float32),
                pltpu.VMEM((n_stage, score_rows, 128), jnp.float32),
                pltpu.SemaphoreType.DMA((NSLOT,)),
                pltpu.SemaphoreType.DMA((NSLOT,)),
                pltpu.SemaphoreType.DMA((n_units, 2, 3)),
                pltpu.SemaphoreType.DMA((n_units, 2, 3)),
                pltpu.SemaphoreType.DMA((2, 2)),
                pltpu.SemaphoreType.DMA((2, 2)),
                pltpu.SemaphoreType.DMA((6,)),
                pltpu.SemaphoreType.DMA((n_tp,)),
                pltpu.SemaphoreType.DMA,
                pltpu.SemaphoreType.DMA((n_batch,)),
                pltpu.SemaphoreType.DMA((2,)),
                pltpu.SemaphoreType.DMA((2,)),
                pltpu.SemaphoreType.DMA((n_stage,)),
                pltpu.SemaphoreType.DMA((n_stage,)),
            ],
            compiler_params=pltpu.CompilerParams(
                collective_id=0, has_side_effects=True, vmem_limit_bytes=VMEM_LIMIT
            ),
            name="layer",
        )(positions.reshape(1, n_seq), rope_rows(), *norm_params, hidden, w_q, w_k, w_v, w_o, w_up, w_down)
        y, neuron, embed, head = pl.pallas_call(
            functools.partial(final_kernel, n_rows, e_rows),
            out_shape=(
                jax.ShapeDtypeStruct(hidden.shape, jnp.bfloat16),
                jax.ShapeDtypeStruct((n_rows, 128), jnp.float32),
                jax.ShapeDtypeStruct((e_rows, 128), jnp.float32),
                jax.ShapeDtypeStruct((1, heads_local), jnp.float32),
            ),
            in_specs=[any_spec, any_spec],
            out_specs=(any_spec, any_spec, any_spec, any_spec),
            scratch_shapes=[
                pltpu.VMEM(hidden.shape, jnp.bfloat16),
                pltpu.VMEM((score_rows, 128), jnp.float32),
                pltpu.VMEM((1, heads_local), jnp.float32),
                pltpu.SemaphoreType.DMA((n_batch + 1,)),
                pltpu.SemaphoreType.DMA((n_batch + 3,)),
            ],
            name="final",
        )(y, score)
        return y, neuron.reshape(ff_local), head.reshape(heads_local), embed.reshape(width)

    weight_col = P(None, "tp")
    weight_row = P("tp", None)
    return jax.shard_map(
        local_layer,
        mesh=mesh,
        in_specs=(P("dp"), P(), P(), P(), weight_col, weight_col, weight_col, weight_row, P(), P(), weight_col, weight_row),
        out_specs=(P("dp"), P("tp"), P("tp"), P()),
        check_vma=False,
    )
```

```python
import functools

import jax
import jax.numpy as jnp
import numpy as np
from jax import lax
from jax.experimental import pallas as pl
from jax.experimental.pallas import tpu as pltpu
from jax.sharding import PartitionSpec as P

HEAD_DIM = 128
ROT_DIM = 64
ROPE_BASE = 10000.0
LN_EPS = 1e-5
TILE = 512
NSLOT = 4
VMEM_LIMIT = 66_000_000
MESH = pl.DeviceIdType.MESH

PROGRAM = (
    ("qkv", 0, 0), ("att", 0, 0), ("o", 0, 0), ("early", "rs1", 0), ("o", 0, 1), ("begin", "rs1", 0), ("mean", 0, 0),
    ("qkv", 1, 0), ("att", 1, 0), ("mid", "rs1", 0), ("o", 1, 0), ("o", 1, 1), ("begin", "rs1", 1), ("mean", 1, 0),
    ("qkv", 2, 0), ("att", 2, 0), ("fin", "rs1", 0), ("begin", "ag1", 0), ("o", 2, 0), ("o", 2, 1),
    ("mid", "rs1", 1), ("mean", 2, 0), ("qkv", 3, 0), ("begin", "rs1", 2), ("att", 3, 0), ("o", 3, 0), ("o", 3, 1),
    ("mid", "ag1", 0), ("mean", 3, 0), ("begin", "rs1", 3), ("fin", "rs1", 1), ("mid", "rs1", 2),
    ("begin", "ag1", 1), ("fin", "ag1", 0), ("up", 0, 0), ("mid", "rs1", 3), ("up", 0, 1), ("dn", 0, 0),
    ("dn", 0, 1), ("fin", "rs1", 2), ("mid", "ag1", 1), ("begin", "ag1", 2), ("begin", "rs2", 0), ("fin", "rs1", 3),
    ("fin", "ag1", 1), ("up", 1, 0), ("mid", "ag1", 2), ("up", 1, 1), ("begin", "ag1", 3), ("dn", 1, 0),
    ("dn", 1, 1), ("mid", "rs2", 0), ("begin", "rs2", 1), ("fin", "ag1", 2), ("up", 2, 0), ("mid", "ag1", 3),
    ("up", 2, 1), ("dn", 2, 0), ("dn", 2, 1), ("fin", "rs2", 0), ("mid", "rs2", 1), ("begin", "ag2", 0),
    ("begin", "rs2", 2), ("fin", "ag1", 3), ("up", 3, 0), ("fin", "rs2", 1), ("up", 3, 1), ("score", 0, 0),
    ("mid", "ag2", 0), ("dn", 3, 0), ("begin", "ag2", 1), ("score", 1, 0), ("dn", 3, 1), ("mid", "rs2", 2),
    ("begin", "rs2", 3), ("score", 2, 0), ("fin", "ag2", 0), ("mid", "ag2", 1), ("fin", "rs2", 2), ("score", 3, 0),
    ("begin", "ag2", 2), ("mid", "rs2", 3), ("fin", "ag2", 1), ("score", 4, 0), ("mid", "ag2", 2), ("fin", "rs2", 3),
    ("begin", "ag2", 3), ("score", 5, 0), ("fin", "ag2", 2), ("mid", "ag2", 3), ("fin", "ag2", 3),
)
UNITS = tuple((op[1], op[2]) for op in PROGRAM if op[0] == "begin")
N_TILES = {"qkv": 4, "o": 2, "up": 4, "dn": 4}


def rope_rows():
    half_rot = ROT_DIM // 2
    lane = np.arange(HEAD_DIM)
    inv_freq = np.where(lane < ROT_DIM, ROPE_BASE ** (-2.0 * (lane % half_rot) / ROT_DIM), 0.0)
    return np.stack([inv_freq, np.where(lane < half_rot, -1.0, 1.0)]).astype(np.float32)


def layer_kernel(
    n_tp, n_dp, pos_in, freq_in, gain1_in, bias1_in, gain2_in, bias2_in,
    hid_ref, wq_ref, wk_ref, wv_ref, wo_ref, wup_ref, wdn_ref,
    y_ref, score_ref,
    wbuf, part, rbuf, gath, hin, qkv, attn, hmid, act, xmid, ystage, pos_ref, freq_ref, rope_ref, raw_ref, norm_ref, nsq, esq, hsq, sbuf, xbuf,
    wsem, vsem, ssem, rsem, esend, erecv, psem, bsem, osem, hsem, xsem, ysem, xssem, xrsem,
):
    me = lax.axis_index("tp")
    my_dp = lax.axis_index("dp")
    right = lax.rem(me + 1, n_tp)
    left = lax.rem(me + n_tp - 1, n_tp)
    opp = lax.rem(me + 2, n_tp)
    n_seq = part.shape[1]
    width = part.shape[2]
    blk = n_seq // n_tp
    half = blk // 2
    k_o = wo_ref.shape[0]
    partners = []
    step = 1
    while step < n_dp:
        bit = lax.rem(my_dp // step, 2)
        partners.append(my_dp + step - 2 * step * bit)
        step *= 2

    def half_rows(owner, which):
        return pl.ds(pl.multiple_of(owner * blk + which * half, half), half)

    pieces = [op for op in PROGRAM if op[0] in N_TILES]
    n_q = wq_ref.shape[1]
    n_kv = wk_ref.shape[1]
    n_qkv = n_q + 2 * n_kv
    q_tiles = n_q // TILE
    group = n_q // n_kv
    bases = {}
    base = 0
    for piece in pieces:
        bases[piece] = base
        base += N_TILES[piece[0]]

    def tile_slot(piece, i):
        return lax.rem(bases[piece] + i, NSLOT)

    def columns(i):
        return pl.ds(pl.multiple_of(i * TILE, TILE), TILE)

    def tile_copies(piece, i):
        kind, _, part_no = piece
        slot = tile_slot(piece, i)
        if kind == "o":
            first = 2 * (N_TILES[kind] * part_no + i)
            return (
                pltpu.make_async_copy(wo_ref.at[:, columns(first)], wbuf.at[slot, pl.ds(0, k_o), :], wsem.at[slot]),
                pltpu.make_async_copy(
                    wo_ref.at[:, columns(first + 1)], wbuf.at[slot, pl.ds(k_o, k_o), :], vsem.at[slot]
                ),
            )
        src = {"qkv": wq_ref, "up": wup_ref, "dn": wdn_ref}[kind]
        tile = N_TILES[kind] * part_no + i
        return (pltpu.make_async_copy(src.at[:, columns(tile)], wbuf.at[slot], wsem.at[slot]),)

    def kv_copies(piece):
        slot = tile_slot(piece, q_tiles)
        return (
            pltpu.make_async_copy(wk_ref, wbuf.at[slot, :, pl.ds(0, n_kv)], wsem.at[slot]),
            pltpu.make_async_copy(wv_ref, wbuf.at[slot, :, pl.ds(n_kv, n_kv)], vsem.at[slot]),
        )

    def start_all(copies_of_tile):
        for copy in copies_of_tile:
            copy.start()

    def start_tile(number):
        for piece in pieces:
            tile = number - bases[piece]
            if 0 <= tile < N_TILES[piece[0]]:
                is_kv = piece[0] == "qkv" and tile == q_tiles
                start_all(kv_copies(piece) if is_kv else tile_copies(piece, tile))

    def look_ahead(piece, i):
        if isinstance(i, int):
            start_tile(bases[piece] + i + NSLOT)
            return
        for j in range(q_tiles if piece[0] == "qkv" else N_TILES[piece[0]]):

            @pl.when(i == j)
            def _(j=j):
                start_tile(bases[piece] + j + NSLOT)

    def norm_rows(rows, which):
        mean = jnp.sum(rows, axis=-1, keepdims=True) * (1.0 / width)
        centered = rows - mean
        var = jnp.sum(centered * centered, axis=-1, keepdims=True) * (1.0 / width)
        scaled = centered * lax.rsqrt(var + LN_EPS)
        out = scaled * norm_ref[pl.ds(2 * which, 1), :] + norm_ref[pl.ds(2 * which + 1, 1), :]
        return out.astype(jnp.bfloat16)

    def seq_copy(seq):
        return pltpu.make_async_copy(hid_ref.at[seq], ystage.at[seq % 2], xsem.at[seq % 2])

    def first_norm(seq):
        seq_copy(seq).wait()

        def rows_body(i, carry):
            rows = pl.ds(pl.multiple_of(i * 16, 16), 16)
            hin[rows, :] = norm_rows(ystage[seq % 2, rows, :].astype(jnp.float32), 0)
            return carry

        lax.fori_loop(0, n_seq // 16, rows_body, 0, unroll=4)
        if seq + 2 < hid_ref.shape[0]:
            seq_copy(seq + 2).start()

    def first_means():
        def cols_body(i, carry):
            cols = pl.ds(pl.multiple_of(i * TILE, TILE), TILE)
            mean = jnp.sum(hin[:, cols].astype(jnp.float32), axis=0, keepdims=True) * (1.0 / n_seq)
            esq[:, cols] += mean * mean
            return carry

        lax.fori_loop(0, width // TILE, cols_body, 0)

    def rotate(raw, lane):
        rot_half = ROT_DIM // 2
        val = raw.astype(jnp.float32)
        ahead = pltpu.roll(val, HEAD_DIM - rot_half, 1)
        behind = pltpu.roll(val, rot_half, 1)
        partner = jnp.where(lane < rot_half, ahead, behind)
        return (val * rope_ref[0] + partner * rope_ref[1]).astype(jnp.bfloat16)

    def attend():
        lane = lax.broadcasted_iota(jnp.int32, (n_seq, HEAD_DIM), 1)
        row = lax.broadcasted_iota(jnp.int32, (n_seq, n_seq), 0)
        col = lax.broadcasted_iota(jnp.int32, (n_seq, n_seq), 1)
        lane_row = lax.broadcasted_iota(jnp.int32, (1, HEAD_DIM), 1)

        def group_body(g, carry):
            def head_cols(start):
                return pl.ds(pl.multiple_of(start, HEAD_DIM), HEAD_DIM)

            keys = rotate(qkv[:, head_cols(n_q + g * HEAD_DIM)], lane)
            vals = qkv[:, head_cols(n_q + n_kv + g * HEAD_DIM)]
            queries = jnp.concatenate(
                [rotate(qkv[:, head_cols((g * group + i) * HEAD_DIM)], lane) for i in range(group)], axis=0
            )
            scores = lax.dot_general(
                queries, keys, (((1,), (1,)), ((), ())), preferred_element_type=jnp.float32
            ) * HEAD_DIM ** -0.5
            probs = []
            for i in range(group):
                masked = jnp.where(row >= col, scores[i * n_seq : (i + 1) * n_seq], -1e30)
                exps = jnp.exp(masked - jnp.max(masked, axis=-1, keepdims=True))
                probs.append((exps * (1.0 / jnp.sum(exps, axis=-1, keepdims=True))).astype(jnp.bfloat16))
            outs = jnp.dot(
                jnp.concatenate(probs, axis=0), vals, preferred_element_type=jnp.float32
            ).astype(jnp.bfloat16)
            head_sum = jnp.zeros((1, HEAD_DIM), jnp.float32)
            for i in range(group):
                out = outs[i * n_seq : (i + 1) * n_seq]
                attn[:, head_cols((g * group + i) * HEAD_DIM)] = out
                out32 = out.astype(jnp.float32)
                norm = jnp.sqrt(jnp.sum(out32 * out32, axis=-1, keepdims=True))
                mean = jnp.sum(norm, axis=0, keepdims=True) * (1.0 / n_seq)
                head_sum += jnp.where(lane_row == g * group + i, mean * mean, 0.0)
            hsq[...] += head_sum
            return carry

        lax.fori_loop(0, n_kv // HEAD_DIM, group_body, 0)

    def run_piece(piece):
        kind, seq, part_no = piece
        if kind == "qkv":
            first_norm(seq)

        def body(i, carry):
            for copy in tile_copies(piece, i):
                copy.wait()
            slot = tile_slot(piece, i)
            tile = N_TILES[kind] * part_no + i
            if kind == "qkv":
                qkv[:, columns(i)] = jnp.dot(
                    hin[...], wbuf[slot], preferred_element_type=jnp.float32
                ).astype(jnp.bfloat16)
            elif kind == "o":
                for j in range(2):
                    part[seq % 3, :, columns(2 * tile + j)] = jnp.dot(
                        attn[...], wbuf[slot, pl.ds(j * k_o, k_o), :], preferred_element_type=jnp.float32
                    )
            elif kind == "up":
                up = jnp.maximum(jnp.dot(hmid[...], wbuf[slot], preferred_element_type=jnp.float32), 0.0)
                sq = up * up
                mean = jnp.sum(sq, axis=0, keepdims=True) * (1.0 / n_seq)
                nsq[:, columns(tile)] += mean * mean
                act[:, columns(tile)] = sq.astype(jnp.bfloat16)
            else:
                part[(4 + seq) % 3, :, columns(tile)] = jnp.dot(
                    act[...], wbuf[slot], preferred_element_type=jnp.float32
                )
            look_ahead(piece, i)
            return carry

        lax.fori_loop(0, q_tiles if kind == "qkv" else N_TILES[kind], body, 0)
        if kind == "qkv":
            if seq == 0:
                read_rope()
            for copy in kv_copies(piece):
                copy.wait()
            qkv[:, pl.ds(n_q, 2 * n_kv)] = jnp.dot(
                hin[...], wbuf[tile_slot(piece, q_tiles)], preferred_element_type=jnp.float32
            ).astype(jnp.bfloat16)
            look_ahead(piece, q_tiles)

    def remote(src, dst, k, direction, j):
        return pltpu.make_async_remote_copy(
            src_ref=src, dst_ref=dst, send_sem=ssem.at[k, direction, j], recv_sem=rsem.at[k, direction, j],
            device_id={"tp": right if direction == 0 else left}, device_id_type=MESH,
        )

    def unit_copies(k):
        kind, seq = UNITS[k]
        ix = seq if kind[2] == "1" else 4 + seq
        if kind[:2] == "rs":
            p = ix % 3
            routes = (
                ((opp, 0), (right, 1), (right, 0)),
                ((opp, 1), (left, 0), (left, 1)),
            )
            return [
                [
                    remote(part.at[p, half_rows(*routes[d][j]), :], rbuf.at[ix, d, j], k, d, j)
                    for j in range(3)
                ]
                for d in range(2)
            ]
        routes = (
            ((me, 0), (me, 1), (left, 0)),
            ((me, 1), (me, 0), (right, 1)),
        )
        return [
            [
                remote(
                    gath.at[ix, half_rows(*routes[d][j]), :], gath.at[ix, half_rows(*routes[d][j]), :], k, d, j
                )
                for j in range(3)
            ]
            for d in range(2)
        ]

    copies = [unit_copies(k) for k in range(len(UNITS))]

    def early_copies():
        def one(d, side):
            rows = half_rows(opp, d)
            cols = pl.ds(side * (width // 2), width // 2)
            sems = (esend.at[d], erecv.at[d]) if side == 0 else (ssem.at[0, d, 0], rsem.at[0, d, 0])
            return pltpu.make_async_remote_copy(
                src_ref=part.at[0, rows, cols], dst_ref=rbuf.at[0, d, 0, :, cols],
                send_sem=sems[0], recv_sem=sems[1],
                device_id={"tp": right if d == 0 else left}, device_id_type=MESH,
            )

        return [[one(d, side) for d in range(2)] for side in range(2)]

    early, late = early_copies()
    for d in range(2):
        copies[0][d][0] = late[d]

    def begin(k):
        for j in range(2):
            for d in range(2):
                copies[k][d][j].start()

    def middle(k):
        kind, seq = UNITS[k]
        ix = seq if kind[2] == "1" else 4 + seq
        for d in range(2):
            if k == 0:
                early[d].wait_recv()
            copies[k][d][0].wait_recv()
            if kind[:2] == "rs":
                rows = half_rows(right if d == 0 else left, d)
                part[ix % 3, rows, :] = part[ix % 3, rows, :] + rbuf[ix, d, 0]
            copies[k][d][2].start()

    def finish(k):
        kind, seq = UNITS[k]
        ix = seq if kind[2] == "1" else 4 + seq
        if k == len(UNITS) - 1:
            last_finish(k, seq, ix)
            return
        for d in range(2):
            for j in (1, 2):
                copies[k][d][j].wait_recv()
        if kind[:2] == "rs":
            for w in range(2):
                rows = half_rows(me, w)
                total = part[ix % 3, rows, :] + rbuf[ix, w, 2] + rbuf[ix, 1 - w, 1]
                mine = pl.ds(w * half, half)
                mid = (xmid[seq, mine, :].astype(jnp.float32) + total).astype(jnp.bfloat16)
                if kind == "rs1":
                    xmid[seq, mine, :] = mid
                    gath[ix, rows, :] = norm_rows(mid.astype(jnp.float32), 1).astype(jnp.float32)
                else:
                    gath[ix, rows, :] = mid.astype(jnp.float32)
        elif kind == "ag1":
            def cast(i, carry):
                cols = pl.ds(pl.multiple_of(i * TILE, TILE), TILE)
                got = gath[ix, :, cols]
                mean = jnp.sum(got, axis=0, keepdims=True) * (1.0 / n_seq)
                esq[:, cols] += mean * mean
                hmid[:, cols] = got.astype(jnp.bfloat16)
                return carry

            lax.fori_loop(0, width // TILE, cast, 0)
        else:
            if seq >= 2:
                y_copy(seq - 2).wait()

            def store(i, carry):
                cols = pl.ds(pl.multiple_of(i * TILE, TILE), TILE)
                ystage[seq % 2, :, cols] = gath[ix, :, cols].astype(jnp.bfloat16)
                return carry

            lax.fori_loop(0, width // TILE, store, 0)
            y_copy(seq).start()
        for d in range(2):
            for j in range(3):
                copies[k][d][j].wait_send()
                if k == 0 and j == 0:
                    early[d].wait_send()

    def block_copy(seq, owner, i):
        rows = pl.ds(pl.multiple_of(owner * blk, blk), blk)
        return pltpu.make_async_copy(ystage.at[seq % 2, rows, :], y_ref.at[seq, rows, :], bsem.at[i])

    def last_finish(k, seq, ix):
        y_copy(seq - 2).wait()
        for i, owner in enumerate((me, left, right, opp)):
            rows = pl.ds(pl.multiple_of(owner * blk, blk), blk)
            if i == 1 or i == 3:
                for d in range(2):
                    copies[k][d][1 if i == 1 else 2].wait_recv()

            def store(c, carry, rows=rows):
                ystage[seq % 2, rows, columns(c)] = gath[ix, rows, columns(c)].astype(jnp.bfloat16)
                return carry

            lax.fori_loop(0, width // TILE, store, 0)
            block_copy(seq, owner, i).start()
        for d in range(2):
            for j in range(3):
                copies[k][d][j].wait_send()
        for i, owner in enumerate((me, left, right, opp)):
            block_copy(seq, owner, i).wait()

    def y_copy(seq):
        return pltpu.make_async_copy(ystage.at[seq % 2], y_ref.at[seq], ysem.at[seq % 2])

    def score_copy(i):
        return pltpu.make_async_remote_copy(
            src_ref=sbuf.at[i], dst_ref=xbuf.at[i], send_sem=xssem.at[i], recv_sem=xrsem.at[i],
            device_id={"dp": partners[i]}, device_id_type=MESH,
        )

    def score_begin():
        n_rows, e_rows = nsq.shape[1] // 128, width // 128
        for r in range(n_rows):
            sbuf[0, r : r + 1, :] = nsq[:, r * 128 : (r + 1) * 128]
        for r in range(e_rows):
            sbuf[0, n_rows + r : n_rows + r + 1, :] = esq[:, r * 128 : (r + 1) * 128]
        sbuf[0, n_rows + e_rows :, :] = jnp.broadcast_to(hsq[...], (8, 128))
        score_copy(0).start()

    def score_step(i):
        score_copy(i).wait()
        sbuf[i + 1] = sbuf[i] + xbuf[i]
        if i + 1 < len(partners):
            score_copy(i + 1).start()

    def read_norm(which):
        for i in (2 * which, 2 * which + 1):
            param_copies[i].wait()
        gain = 1.0 + raw_ref[2 * which].astype(jnp.float32)
        bias = raw_ref[2 * which + 1].astype(jnp.float32)
        for r in range(width // 128):
            cols = slice(r * 128, (r + 1) * 128)
            norm_ref[2 * which : 2 * which + 1, cols] = gain[r : r + 1, :]
            norm_ref[2 * which + 1 : 2 * which + 2, cols] = bias[r : r + 1, :]

    def read_rope():
        for copy in param_copies[4:]:
            copy.wait()
        row = lax.broadcasted_iota(jnp.int32, (n_seq, n_seq), 0)
        col = lax.broadcasted_iota(jnp.int32, (n_seq, n_seq), 1)
        pos = jnp.where(row == col, pos_ref[...].astype(jnp.float32), 0.0)
        angle = jnp.sum(pos, axis=1, keepdims=True) * freq_ref[0:1, :]
        rope_ref[0] = jnp.cos(angle)
        rope_ref[1] = freq_ref[1:2, :] * jnp.sin(angle)

    param_copies = [
        pltpu.make_async_copy(src, raw_ref.at[i], psem.at[i])
        for i, src in enumerate((gain1_in, bias1_in, gain2_in, bias2_in))
    ] + [
        pltpu.make_async_copy(pos_in, pos_ref, psem.at[4]),
        pltpu.make_async_copy(freq_in, freq_ref, psem.at[5]),
    ]
    hid_copies = [
        pltpu.make_async_copy(
            hid_ref.at[seq, pl.ds(pl.multiple_of(me * blk, blk), blk), :], xmid.at[seq], hsem.at[seq]
        )
        for seq in range(hid_ref.shape[0])
    ]
    seq_copy(0).start()
    start_all(param_copies)
    start_tile(0)
    for i in range(1, NSLOT):
        start_tile(i)

    barrier = pltpu.get_barrier_semaphore()
    for t in (left, right):
        pl.semaphore_signal(barrier, inc=1, device_id={"tp": t}, device_id_type=MESH)
    for other in partners:
        pl.semaphore_signal(barrier, inc=1, device_id={"dp": other}, device_id_type=MESH)
    read_norm(0)
    nsq[...] = jnp.zeros_like(nsq)
    esq[...] = jnp.zeros_like(esq)
    hsq[...] = jnp.zeros_like(hsq)

    score_out = pltpu.make_async_copy(sbuf.at[0], score_ref, osem)
    for op in PROGRAM:
        name, arg, no = op
        if name in N_TILES:
            run_piece(op)
        elif name == "att":
            if arg == 0:
                seq_copy(1).start()
            attend()
        elif name == "early":
            pl.semaphore_wait(barrier, 2 + len(partners))
            start_all(early)
        elif name == "mean":
            first_means()
        elif name == "begin":
            k = UNITS.index((arg, no))
            begin(k)
            if k == 0:
                start_all(hid_copies)
        elif name == "mid":
            middle(UNITS.index((arg, no)))
        elif name == "fin":
            if (arg, no) == UNITS[0]:
                read_norm(1)
                for copy in hid_copies:
                    copy.wait()
            finish(UNITS.index((arg, no)))
        elif arg == 0:
            score_begin()
        else:
            score_step(arg - 1)
            if arg == len(partners):
                sbuf[0] = jnp.sqrt(sbuf[len(partners)])
                score_out.start()
    y_copy(2).wait()
    score_out.wait()


def final_kernel(
    n_rows, e_rows, y_ref, score_ref, out_ref, neuron_ref, embed_ref, head_ref, stage, scores, heads, in_sem, out_sem
):
    count = y_ref.shape[0]
    loads = [pltpu.make_async_copy(y_ref.at[i], stage.at[i], in_sem.at[i]) for i in range(count)]
    stores = [pltpu.make_async_copy(stage.at[i], out_ref.at[i], out_sem.at[i]) for i in range(count)]
    loads.insert(0, pltpu.make_async_copy(score_ref, scores, in_sem.at[count]))
    score_stores = [
        pltpu.make_async_copy(scores.at[pl.ds(0, n_rows), :], neuron_ref, out_sem.at[count]),
        pltpu.make_async_copy(scores.at[pl.ds(n_rows, e_rows), :], embed_ref, out_sem.at[count + 1]),
        pltpu.make_async_copy(heads, head_ref, out_sem.at[count + 2]),
    ]
    for load in loads:
        load.start()
    loads[0].wait()
    heads[...] = scores[n_rows + e_rows : n_rows + e_rows + 1, : heads.shape[1]]
    for store in score_stores:
        store.start()
    for load, store in zip(loads[1:], stores):
        load.wait()
        store.start()
    for store in score_stores + stores:
        store.wait()


def solution(mesh):
    n_tp = mesh.shape["tp"]
    n_dp = mesh.shape["dp"]

    def local_layer(hidden, positions, ln1_gain, ln1_bias, w_q, w_k, w_v, w_o, ln2_gain, ln2_bias, w_up, w_down):
        n_batch, n_seq, width = hidden.shape
        ff_local = w_up.shape[1]
        heads_local = w_q.shape[1] // HEAD_DIM
        norm_params = [p.reshape(width // 128, 128) for p in (ln1_gain, ln1_bias, ln2_gain, ln2_bias)]
        n_rows, e_rows = ff_local // 128, width // 128
        score_rows = n_rows + e_rows + 8
        n_stage = n_dp.bit_length() - 1
        blk = n_seq // n_tp
        any_spec = pl.BlockSpec(memory_space=pl.ANY)
        n_units = len(UNITS)
        y, score = pl.pallas_call(
            functools.partial(layer_kernel, n_tp, n_dp),
            out_shape=(
                jax.ShapeDtypeStruct(hidden.shape, jnp.bfloat16),
                jax.ShapeDtypeStruct((score_rows, 128), jnp.float32),
            ),
            in_specs=[any_spec] * 13,
            out_specs=(any_spec, any_spec),
            scratch_shapes=[
                pltpu.VMEM((NSLOT, width, TILE), jnp.bfloat16),
                pltpu.VMEM((3, n_seq, width), jnp.float32),
                pltpu.VMEM((2 * n_batch, 2, 3, blk // 2, width), jnp.float32),
                pltpu.VMEM((2 * n_batch, n_seq, width), jnp.float32),
                pltpu.VMEM((n_seq, width), jnp.bfloat16),
                pltpu.VMEM((n_seq, w_q.shape[1] + 2 * w_k.shape[1]), jnp.bfloat16),
                pltpu.VMEM((n_seq, w_q.shape[1]), jnp.bfloat16),
                pltpu.VMEM((n_seq, width), jnp.bfloat16),
                pltpu.VMEM((n_seq, ff_local), jnp.bfloat16),
                pltpu.VMEM((n_batch, blk, width), jnp.bfloat16),
                pltpu.VMEM((2, n_seq, width), jnp.bfloat16),
                pltpu.VMEM((1, n_seq), jnp.int32),
                pltpu.VMEM((2, HEAD_DIM), jnp.float32),
                pltpu.VMEM((2, n_seq, HEAD_DIM), jnp.float32),
                pltpu.VMEM((4, width // 128, 128), jnp.bfloat16),
                pltpu.VMEM((4, width), jnp.float32),
                pltpu.VMEM((1, ff_local), jnp.float32),
                pltpu.VMEM((1, width), jnp.float32),
                pltpu.VMEM((1, 128), jnp.float32),
                pltpu.VMEM((n_stage + 1, score_rows, 128), jnp.float32),
                pltpu.VMEM((n_stage, score_rows, 128), jnp.float32),
                pltpu.SemaphoreType.DMA((NSLOT,)),
                pltpu.SemaphoreType.DMA((NSLOT,)),
                pltpu.SemaphoreType.DMA((n_units, 2, 3)),
                pltpu.SemaphoreType.DMA((n_units, 2, 3)),
                pltpu.SemaphoreType.DMA((2,)),
                pltpu.SemaphoreType.DMA((2,)),
                pltpu.SemaphoreType.DMA((6,)),
                pltpu.SemaphoreType.DMA((n_tp,)),
                pltpu.SemaphoreType.DMA,
                pltpu.SemaphoreType.DMA((n_batch,)),
                pltpu.SemaphoreType.DMA((2,)),
                pltpu.SemaphoreType.DMA((2,)),
                pltpu.SemaphoreType.DMA((n_stage,)),
                pltpu.SemaphoreType.DMA((n_stage,)),
            ],
            compiler_params=pltpu.CompilerParams(
                collective_id=0, has_side_effects=True, vmem_limit_bytes=VMEM_LIMIT
            ),
            name="layer",
        )(positions.reshape(1, n_seq), rope_rows(), *norm_params, hidden, w_q, w_k, w_v, w_o, w_up, w_down)
        y, neuron, embed, head = pl.pallas_call(
            functools.partial(final_kernel, n_rows, e_rows),
            out_shape=(
                jax.ShapeDtypeStruct(hidden.shape, jnp.bfloat16),
                jax.ShapeDtypeStruct((n_rows, 128), jnp.float32),
                jax.ShapeDtypeStruct((e_rows, 128), jnp.float32),
                jax.ShapeDtypeStruct((1, heads_local), jnp.float32),
            ),
            in_specs=[any_spec, any_spec],
            out_specs=(any_spec, any_spec, any_spec, any_spec),
            scratch_shapes=[
                pltpu.VMEM(hidden.shape, jnp.bfloat16),
                pltpu.VMEM((score_rows, 128), jnp.float32),
                pltpu.VMEM((1, heads_local), jnp.float32),
                pltpu.SemaphoreType.DMA((n_batch + 1,)),
                pltpu.SemaphoreType.DMA((n_batch + 3,)),
            ],
            name="final",
        )(y, score)
        return y, neuron.reshape(ff_local), head.reshape(heads_local), embed.reshape(width)

    weight_col = P(None, "tp")
    weight_row = P("tp", None)
    return jax.shard_map(
        local_layer,
        mesh=mesh,
        in_specs=(P("dp"), P(), P(), P(), weight_col, weight_col, weight_col, weight_row, P(), P(), weight_col, weight_row),
        out_specs=(P("dp"), P("tp"), P("tp"), P()),
        check_vma=False,
    )
```
